8 devices in a mesh: data: 8 (over z, y, x, core).
Axes of the slice: x: 2, y: 2, z: 1, core: 2. Of those that a mesh axis runs over, the one named last changes fastest.
Arguments:
- h_a: bfloat16 [4096, 384], P('data')
- h_b: bfloat16 [4096, 384], P('data')
- w_one: bfloat16 [384, 2048], replicated
- w_two: bfloat16 [2048, 2048], replicated
- w_three: bfloat16 [2048, 2048], replicated
- gain_one: float32 [2048], replicated
- shift_one: float32 [2048], replicated
- gain_two: float32 [2048], replicated
- shift_two: float32 [2048], replicated
- lam_off: float32 [], replicated
Outputs:
- output 1: float32 [], replicated
- output 2: float32 [384, 2048], P('data')
- output 3: float32 [2048, 2048], P('data')
- output 4: float32 [2048, 2048], P('data')
- output 5: float32 [2048], replicated
- output 6: float32 [2048], replicated
- output 7: float32 [2048], replicated
- output 8: float32 [2048], replicated
All inputs are finite; a program needn't handle non-finite values.
Results may differ from the reference program's by a relative error of at most 0.00504015.
Values are sent between devices in bfloat16 or wider.
A program may use at most 1 GiB of HBM per device.

```python
import jax
import jax.numpy as jnp
from jax import lax

FEAT_DIM = 384
PROJ_DIM = 2048
ROWS_DEV = 512
SHARDS = 8
TOTAL_ROWS = ROWS_DEV * SHARDS
NORM_EPS = 1e-5


def setup_inputs(seed: int = 0) -> dict:
    key_list = jax.random.split(jax.random.key(seed), 14)
    common = jax.random.normal(key_list[0], (TOTAL_ROWS, FEAT_DIM), jnp.float32)
    shard_shift = 0.6 * jax.random.normal(key_list[1], (SHARDS, 1, FEAT_DIM), jnp.float32)
    shard_scale = jnp.exp(0.3 * jax.random.normal(key_list[2], (SHARDS, 1, FEAT_DIM), jnp.float32))

    def make_view(view_key):
        noise_vals = jax.random.normal(view_key, (TOTAL_ROWS, FEAT_DIM), jnp.float32)
        mixed_rows = (0.77 * common + 0.64 * noise_vals).reshape(SHARDS, ROWS_DEV, FEAT_DIM)
        return (mixed_rows * shard_scale + shard_shift).reshape(TOTAL_ROWS, FEAT_DIM).astype(jnp.bfloat16)

    def make_weight(weight_key, fan_in, fan_out):
        weight_scale = fan_in ** -0.5
        return (jax.random.normal(weight_key, (fan_in, fan_out), jnp.float32) * weight_scale).astype(jnp.bfloat16)

    def make_vector(vec_key, center):
        return center + 0.25 * jax.random.normal(vec_key, (PROJ_DIM,), jnp.float32)

    lam_off = (0.1 + 0.2 * jax.random.uniform(key_list[12], (), jnp.float32)) * TOTAL_ROWS / PROJ_DIM
    return {
        "h_a": make_view(key_list[3]),
        "h_b": make_view(key_list[4]),
        "w_one": make_weight(key_list[5], FEAT_DIM, PROJ_DIM),
        "w_two": make_weight(key_list[6], PROJ_DIM, PROJ_DIM),
        "w_three": make_weight(key_list[7], PROJ_DIM, PROJ_DIM),
        "gain_one": make_vector(key_list[8], 1.0),
        "shift_one": make_vector(key_list[9], 0.0),
        "gain_two": make_vector(key_list[10], 1.0),
        "shift_two": make_vector(key_list[11], 0.0),
        "lam_off": lam_off,
    }


def batch_norm(values):
    col_mean = jnp.sum(values, axis=0) / TOTAL_ROWS
    col_var = jnp.sum(values * values, axis=0) / TOTAL_ROWS - col_mean * col_mean
    return (values - col_mean) * lax.rsqrt(col_var + NORM_EPS)


def project(feat_rows, params):
    w_one, w_two, w_three, gain_one, shift_one, gain_two, shift_two = params
    hidden_one = jnp.dot(feat_rows.astype(jnp.float32), w_one, preferred_element_type=jnp.float32)
    act_one = jax.nn.relu(gain_one * batch_norm(hidden_one) + shift_one).astype(jnp.bfloat16)
    hidden_two = jnp.dot(act_one.astype(jnp.float32), w_two, preferred_element_type=jnp.float32)
    act_two = jax.nn.relu(gain_two * batch_norm(hidden_two) + shift_two).astype(jnp.bfloat16)
    proj_out = jnp.dot(act_two.astype(jnp.float32), w_three, preferred_element_type=jnp.float32)
    return batch_norm(proj_out).astype(jnp.bfloat16)


def barlow_loss(params, h_a, h_b, lam_off):
    embed_a = project(h_a, params).astype(jnp.float32)
    embed_b = project(h_b, params).astype(jnp.float32)
    corr_mat = jnp.dot(embed_a.T, embed_b, preferred_element_type=jnp.float32) / TOTAL_ROWS
    feat_index = jnp.arange(PROJ_DIM)
    diag_mask = feat_index[:, None] == feat_index[None, :]
    diag_gap = 1.0 - jnp.diagonal(corr_mat)
    off_square = jnp.sum(jnp.where(diag_mask, 0.0, corr_mat * corr_mat))
    return jnp.sum(diag_gap * diag_gap) + lam_off * off_square


def reference(h_a, h_b, w_one, w_two, w_three, gain_one, shift_one, gain_two, shift_two, lam_off):
    params = (w_one.astype(jnp.float32), w_two.astype(jnp.float32), w_three.astype(jnp.float32),
              gain_one, shift_one, gain_two, shift_two)
    loss_total, grad_list = jax.value_and_grad(barlow_loss)(params, h_a, h_b, lam_off)
    return (loss_total, grad_list[0], grad_list[1], grad_list[2],
            grad_list[3], grad_list[4], grad_list[5], grad_list[6])
```

```python
import functools

import jax
import jax.numpy as jnp
from jax import lax
from jax.experimental import pallas as pl
from jax.experimental.pallas import tpu as pltpu
from jax.sharding import PartitionSpec as P

MESH = pl.DeviceIdType.MESH
F32, BF16 = jnp.float32, jnp.bfloat16
NORM_EPS = 1e-5
TOTAL_ROWS = 4096
VIEW = 512
ROWS = 2 * VIEW
FEAT = 384
WIDTH = 2048
TILE = 256
TILES = WIDTH // TILE
PIECE = FEAT // 8
LAG_C, LAG_D = 2, 4
PA_SLOTS, R0_SLOTS, R1_SLOTS, R2_SLOTS = 5, 2, 4, 4


def dot_nn(a, b):
    return jnp.dot(a, b, preferred_element_type=F32)


def dot_nt(a, b):
    return lax.dot_general(a, b, (((1,), (1,)), ((), ())), preferred_element_type=F32)


def when_in(cond, fn):
    if isinstance(cond, bool):
        if cond:
            fn()
    else:
        pl.when(cond)(fn)


def peer_of(me, r):
    out = me
    for bit in (1, 2, 4):
        if r & bit:
            out = out + bit - 2 * bit * ((me // bit) % 2)
    return out


def entry_barrier(me):
    barrier = pltpu.get_barrier_semaphore()
    for r in range(1, 8):
        pl.semaphore_signal(barrier, inc=1, device_id=(peer_of(me, r),), device_id_type=MESH)
    pl.semaphore_wait(barrier, 7)


def cols(t, width=TILE):
    if isinstance(t, int):
        return pl.ds(t * width, width)
    return pl.ds(pl.multiple_of(t * width, width), width)


def stats_send(me, st, ssem, rsem, i):
    for r in range(1, 8):
        pltpu.make_async_remote_copy(
            src_ref=st.at[i, 0], dst_ref=st.at[i, r], send_sem=ssem.at[i], recv_sem=rsem.at[i],
            device_id=(peer_of(me, r),), device_id_type=MESH).start()


def stats_wait(st, ssem, rsem, i):
    block = st.at[i, pl.ds(1, 7)]
    pltpu.make_async_copy(block, block, rsem.at[i]).wait()
    pltpu.make_async_copy(block, block, ssem.at[i]).wait()


def stats_total(st, i):
    pairs = [st[i, 2 * k] + st[i, 2 * k + 1] for k in range(4)]
    return (pairs[0] + pairs[1]) + (pairs[2] + pairs[3])


def stats_put(st, i, values, weighted):
    rows = []
    for v in range(2):
        part = slice(v * VIEW, (v + 1) * VIEW)
        rows.append(jnp.sum(values[part], axis=0, keepdims=True))
        rows.append(jnp.sum(weighted[part], axis=0, keepdims=True))
    for k in range(4):
        st[i, 0, pl.ds(k, 1), :] = rows[k]


def forward_kernel(h_a, h_b, w1_hbm, w2_hbm, w3_hbm, g1, b1, g2, b2,
                   x1, x2, zh, inv_out, xh1_hbm, xh2_hbm, zn_hbm,
                   w1, wb, u, st, w1_sem, w_sem, out_sem, ssem, rsem):
    me = lax.axis_index("data")
    w1_copy = pltpu.make_async_copy(w1_hbm, w1, w1_sem)
    w1_copy.start()

    def w_copy(layer, q):
        src = (w2_hbm, w3_hbm)[layer]
        return pltpu.make_async_copy(src.at[:, cols(q)], wb.at[layer, q], w_sem.at[layer, q])

    for layer in range(2):
        for q in range(TILES):
            w_copy(layer, q).start()
    entry_barrier(me)
    w1_copy.wait()

    outs_hbm = (xh1_hbm, xh2_hbm, zn_hbm)
    acts = (x1, x2, zh)

    def out_copy(layer, q):
        return pltpu.make_async_copy(u.at[q], outs_hbm[layer].at[q], out_sem.at[q])

    for layer in range(3):
        base = layer * TILES

        def matmul_tile(q, carry, layer=layer, base=base):
            if layer > 0:
                out_copy(layer - 1, q).wait()
                w_copy(layer - 1, q).wait()
                vals = dot_nn(acts[layer - 1][...], wb[layer - 1, q])
            else:
                tile = w1[:, cols(q)]
                vals = jnp.concatenate([dot_nn(h_a[...], tile), dot_nn(h_b[...], tile)], axis=0)
            u[q] = vals
            stats_put(st, base + q, vals, vals * vals)
            stats_send(me, st, ssem, rsem, base + q)
            return carry

        lax.fori_loop(0, TILES, matmul_tile, 0)

        def norm_tile(q, carry, layer=layer, base=base):
            stats_wait(st, ssem, rsem, base + q)
            total = stats_total(st, base + q) * (1.0 / TOTAL_ROWS)
            for v in range(2):
                mean = total[2 * v:2 * v + 1]
                inv = lax.rsqrt(total[2 * v + 1:2 * v + 2] - mean * mean + NORM_EPS)
                inv_out[layer, q, pl.ds(v, 1), :] = inv
                rows = pl.ds(v * VIEW, VIEW)
                normed = (u[q, rows, :] - mean) * inv
                u[q, rows, :] = normed
                if layer < 2:
                    gain, shift = ((g1, b1), (g2, b2))[layer]
                    normed = jnp.maximum(gain[:, cols(q)] * normed + shift[:, cols(q)], 0.0)
                acts[layer][rows, cols(q)] = normed.astype(BF16)
            out_copy(layer, q).start()
            return carry

        lax.fori_loop(0, TILES, norm_tile, 0)
    for q in range(TILES):
        out_copy(2, q).wait()


class Ring:
    def __init__(self, me, items, pa, r0, r1, r2, sems, credits):
        self.items, self.pa, self.r0, self.r1, self.r2 = items, pa, r0, r1, r2
        self.s0, self.q0, self.s1, self.q1, self.s2, self.q2 = sems
        self.c0, self.c1, self.c2 = credits
        core = me % 2
        x, y = (me // 2) % 2, me // 4
        self.core = core
        self.f = x + core * (y - x)
        self.s = y + core * (x - y)
        x_side, y_side = me + 2 - 4 * x, me + 4 - 8 * y
        self.partner = me + 1 - 2 * core
        self.first = x_side + core * (y_side - x_side)
        self.second = y_side + core * (x_side - y_side)

    def copy(self, src, dst, send, recv, device):
        return pltpu.make_async_remote_copy(src_ref=src, dst_ref=dst, send_sem=send, recv_sem=recv,
                                            device_id=(device,), device_id_type=MESH)

    def copy0(self, t, rows):
        return self.copy(self.pa.at[t % PA_SLOTS, 1 - self.core, :, :, pl.ds(0, rows)],
                         self.r0.at[t % R0_SLOTS, :, :, pl.ds(0, rows)],
                         self.s0.at[t % R0_SLOTS], self.q0.at[t % R0_SLOTS], self.partner)

    def copy1(self, t, rows):
        return self.copy(self.pa.at[t % PA_SLOTS, self.core, 1 - self.f, :, pl.ds(0, rows)],
                         self.r1.at[t % R1_SLOTS, :, pl.ds(0, rows)],
                         self.s1.at[t % R1_SLOTS], self.q1.at[t % R1_SLOTS], self.first)

    def copy2(self, t, rows):
        return self.copy(self.pa.at[t % PA_SLOTS, self.core, self.f, 1 - self.s, pl.ds(0, rows)],
                         self.r2.at[t % R2_SLOTS, pl.ds(0, rows)],
                         self.s2.at[t % R2_SLOTS], self.q2.at[t % R2_SLOTS], self.second)

    def take_credit(self, sem, t, slots):
        when_in(t >= slots, lambda: pl.semaphore_wait(sem, 1))

    def give_credit(self, sem, t, slots, device):
        when_in(t + slots < self.items,
                lambda: pl.semaphore_signal(sem, inc=1, device_id=(device,), device_id_type=MESH))

    def send0(self, t, rows=TILE):
        self.take_credit(self.c0, t, R0_SLOTS)
        self.copy0(t, rows).start()

    def stage_b(self, t, rows=TILE):
        self.copy0(t, rows).wait()
        slot = t % PA_SLOTS
        for k in range(4):
            a, b = k // 2, k % 2
            self.pa[slot, self.core, a, b, :rows] += self.r0[t % R0_SLOTS, a, b, :rows]
        self.give_credit(self.c0, t, R0_SLOTS, self.partner)
        self.take_credit(self.c1, t, R1_SLOTS)
        self.copy1(t, rows).start()

    def stage_c(self, t, rows=TILE):
        self.copy1(t, rows).wait()
        slot = t % PA_SLOTS
        for b in range(2):
            self.pa[slot, self.core, self.f, b, :rows] += self.r1[t % R1_SLOTS, b, :rows]
        self.give_credit(self.c1, t, R1_SLOTS, self.first)
        self.take_credit(self.c2, t, R2_SLOTS)
        self.copy2(t, rows).start()

    def stage_d(self, t, rows=TILE):
        self.copy2(t, rows).wait()
        total = self.pa[t % PA_SLOTS, self.core, self.f, self.s, :rows] + self.r2[t % R2_SLOTS, :rows]
        self.give_credit(self.c2, t, R2_SLOTS, self.second)
        return total

    def partial(self, t, lt, right):
        for half in range(2):
            core = self.core if half else 1 - self.core

            def block(k, carry, core=core):
                a, b = k // 2, k % 2
                dev = core + a * (2 + 2 * core) + b * (4 - 2 * core)
                self.pa[t % PA_SLOTS, core, a, b] = dot_nn(lt[...], right(dev))
                return carry

            lax.fori_loop(0, 4, block, 0)
            if half == 0:
                self.send0(t)


RING_SCRATCH = [
    pltpu.VMEM((PA_SLOTS, 2, 2, 2, TILE, TILE), F32),
    pltpu.VMEM((R0_SLOTS, 2, 2, TILE, TILE), F32),
    pltpu.VMEM((R1_SLOTS, 2, TILE, TILE), F32),
    pltpu.VMEM((R2_SLOTS, TILE, TILE), F32),
    pltpu.SemaphoreType.DMA((R0_SLOTS,)), pltpu.SemaphoreType.DMA((R0_SLOTS,)),
    pltpu.SemaphoreType.DMA((R1_SLOTS,)), pltpu.SemaphoreType.DMA((R1_SLOTS,)),
    pltpu.SemaphoreType.DMA((R2_SLOTS,)), pltpu.SemaphoreType.DMA((R2_SLOTS,)),
    pltpu.SemaphoreType.REGULAR, pltpu.SemaphoreType.REGULAR, pltpu.SemaphoreType.REGULAR,
]


LAG_F, LAG_H, LAG_I = 5, 6, 7


def corr_kernel(zh, zn_hbm, inv, lam, dz, loss_out,
                zn, acc, gt, lt, loss_acc, st, zn_sem, ssem, rsem,
                es, er, fs, fr, hs, hr, *ring_refs):
    me = lax.axis_index("data")
    zn_copy = pltpu.make_async_copy(zn_hbm, zn, zn_sem)
    zn_copy.start()
    entry_barrier(me)
    ring = Ring(me, TILES, *ring_refs[:4], ring_refs[4:10], ring_refs[10:])
    core, f, s = ring.core, ring.f, ring.s
    lam_val = lam[0, 0]
    acc[...] = jnp.zeros_like(acc)
    loss_acc[...] = jnp.zeros_like(loss_acc)

    def copy_e(t):
        block = gt.at[t, core, f, s]
        return ring.copy(block, block, es.at[t], er.at[t], ring.second)

    def copy_f(t):
        block = gt.at[t, core, f]
        return ring.copy(block, block, fs.at[t], fr.at[t], ring.first)

    def copy_h(t):
        block = gt.at[t, core]
        return ring.copy(block, block, hs.at[t], hr.at[t], ring.partner)

    def stage_a(t):
        lt[...] = zh[pl.ds(VIEW, VIEW), cols(t)].T
        ring.partial(t, lt, lambda dev: zh[pl.ds(0, VIEW), cols(dev)])
        ring.stage_b(t)

    def stage_d(t):
        corr = ring.stage_d(t) * (1.0 / TOTAL_ROWS)
        diag = (lax.broadcasted_iota(jnp.int32, corr.shape, 0) + TILE * t
                == lax.broadcasted_iota(jnp.int32, corr.shape, 1) + TILE * me)
        gap = 1.0 - corr
        loss_acc[...] += jnp.sum(jnp.where(diag, gap * gap, lam_val * corr * corr), axis=0, keepdims=True)
        grad = jnp.where(diag, -2.0 * gap, (2.0 * lam_val) * corr)
        gt[t, core, f, s] = (grad * (1.0 / TOTAL_ROWS)).astype(BF16)
        copy_e(t).start()

    def stage_f(t):
        copy_e(t).wait()
        copy_f(t).start()

    def stage_h(t):
        copy_f(t).wait()
        copy_h(t).start()

    def stage_i(t):
        copy_h(t).wait()

        def block(k, carry):
            c, a, b = k // 4, (k // 2) % 2, k % 2
            dev = c + a * (2 + 2 * c) + b * (4 - 2 * c)
            grad = gt[t, c, a, b]
            acc[dev, pl.ds(0, VIEW), :] += dot_nn(zh[pl.ds(VIEW, VIEW), cols(t)], grad)
            acc[t, pl.ds(VIEW, VIEW), :] += dot_nt(zh[pl.ds(0, VIEW), cols(dev)], grad)
            return carry

        lax.fori_loop(0, 8, block, 0)

    def tick(t, carry):
        for lag, stage in ((0, stage_a), (LAG_C, ring.stage_c), (LAG_D, stage_d), (LAG_F, stage_f),
                           (LAG_H, stage_h), (LAG_I, stage_i)):
            item = t - lag
            pl.when((item >= 0) & (item < TILES))(functools.partial(stage, item))
        return carry

    lax.fori_loop(0, TILES + LAG_I, tick, 0)
    st[TILES, 0] = jnp.zeros((4, TILE), F32)
    st[TILES, 0, pl.ds(0, 1), :] = loss_acc[...]
    stats_send(me, st, ssem, rsem, TILES)
    zn_copy.wait()

    def sums(q, carry):
        grad = acc[q]
        stats_put(st, q, grad, grad * zn[q])
        stats_send(me, st, ssem, rsem, q)
        return carry

    lax.fori_loop(0, TILES, sums, 0)

    def norm(q, carry):
        stats_wait(st, ssem, rsem, q)
        total = stats_total(st, q) * (1.0 / TOTAL_ROWS)
        for v in range(2):
            rows = pl.ds(v * VIEW, VIEW)
            grad = acc[q, rows, :] - (total[2 * v:2 * v + 1] + zn[q, rows, :] * total[2 * v + 1:2 * v + 2])
            dz[rows, cols(q)] = (inv[2, q, pl.ds(v, 1), :] * grad).astype(BF16)
        return carry

    lax.fori_loop(0, TILES, norm, 0)
    stats_wait(st, ssem, rsem, TILES)
    loss_out[...] = jnp.broadcast_to(jnp.sum(stats_total(st, TILES), keepdims=True), loss_out.shape)


ITEMS = 2 * TILES + 2
LAST_ROWS = 4 * PIECE


def backward_kernel(dz, x2, x1, h_a, h_b, w3_hbm, w2_hbm, xh2_hbm, xh1_hbm, inv, g1, b1, g2, b2,
                    dw_hbm, dw1, sums_out,
                    du2, du1, ht, lt, wt, xh, gpre, stage, st,
                    w_sem, xh_sem, out_sem, ssem, rsem, *ring_refs):
    me = lax.axis_index("data")
    entry_barrier(me)
    ring = Ring(me, ITEMS, *ring_refs[:4], ring_refs[4:10], ring_refs[10:])

    def out_copy(t):
        return pltpu.make_async_copy(stage.at[t % 2], dw_hbm.at[t // TILES, :, cols(t % TILES)], out_sem.at[t % 2])

    def store_out(t):
        when_in(t >= 2, lambda: out_copy(t - 2).wait())
        stage[t % 2] = ring.stage_d(t).T
        out_copy(t).start()

    for g in range(2):
        left, right, grad_out = ((dz, x2, du2), (du2, x1, du1))[g]
        w_hbm, xh_hbm = ((w3_hbm, xh2_hbm), (w2_hbm, xh1_hbm))[g]
        gain_ref, shift_ref = ((g2, b2), (g1, b1))[g]
        base = g * TILES

        def w_copy(e, w_hbm=w_hbm):
            rows = e * TILE if isinstance(e, int) else pl.multiple_of(e * TILE, TILE)
            return pltpu.make_async_copy(w_hbm.at[pl.ds(rows, TILE), :], wt.at[e % 2], w_sem.at[e % 2])

        def xh_copy(e, xh_hbm=xh_hbm):
            return pltpu.make_async_copy(xh_hbm.at[e], xh.at[e % 4], xh_sem.at[e % 4])

        def fetch(e, w_copy=w_copy, xh_copy=xh_copy):
            w_copy(e).start()
            xh_copy(e).start()

        fetch(0)
        fetch(1)

        def grad_tile(e, left=left, w_copy=w_copy, xh_copy=xh_copy, base=base,
                      gain_ref=gain_ref, shift_ref=shift_ref):
            w_copy(e).wait()
            xh_copy(e).wait()
            grad = dot_nt(left[...], wt[e % 2])
            normed = xh[e % 4]
            pre = gain_ref[:, cols(e)] * normed + shift_ref[:, cols(e)]
            grad = jnp.where(pre > 0, grad, 0.0)
            gpre[e % 3] = grad
            stats_put(st, base + e, grad, grad * normed)
            stats_send(me, st, ssem, rsem, base + e)

        def norm_tile(e, g=g, base=base, grad_out=grad_out, gain_ref=gain_ref):
            stats_wait(st, ssem, rsem, base + e)
            total = stats_total(st, base + e)
            for k in range(2):
                sums_out[pl.ds(2 * g + k, 1), cols(e)] = total[k:k + 1] + total[k + 2:k + 3]
            total = total * (1.0 / TOTAL_ROWS)
            for v in range(2):
                rows = pl.ds(v * VIEW, VIEW)
                grad = gpre[e % 3, rows, :] - (
                    total[2 * v:2 * v + 1] + xh[e % 4, rows, :] * total[2 * v + 1:2 * v + 2])
                scale = gain_ref[:, cols(e)] * inv[1 - g, e, pl.ds(v, 1), :]
                grad_out[rows, cols(e)] = (scale * grad).astype(BF16)

        def tick(q, carry, g=g, base=base, left=left, right=right,
                 grad_tile=grad_tile, norm_tile=norm_tile, fetch=fetch):
            t = base + q
            lt[...] = left[:, cols(q)].T
            ring.partial(t, lt, lambda dev: right[:, cols(dev)])

            def step(k, carry):
                e = 2 * q + k
                pl.when(e < TILES)(lambda: grad_tile(e))

                @pl.when(e >= 2)
                def _():
                    norm_tile(e - 2)

                pl.when(e + 2 < TILES)(lambda: fetch(e + 2))
                return carry

            @pl.when(q <= TILES // 2)
            def _():
                lax.fori_loop(0, 2, step, 0)

            ring.stage_b(t)
            pl.when(t >= LAG_C)(lambda: ring.stage_c(t - LAG_C))
            pl.when(t >= LAG_D)(lambda: store_out(t - LAG_D))
            return carry

        lax.fori_loop(0, TILES, tick, 0)

    ht[:, pl.ds(0, VIEW)] = h_a[...].T
    ht[:, pl.ds(VIEW, VIEW)] = h_b[...].T

    def rows_of(t):
        return LAST_ROWS if t >= 2 * TILES else TILE

    for t in range(2 * TILES, ITEMS + LAG_D):
        if t < ITEMS:
            for m in range(4):
                part = dot_nn(ht[...], du1[:, cols((t - 2 * TILES) * 4 + m)])
                for dev in range(8):
                    c, x, y = dev % 2, (dev // 2) % 2, dev // 4
                    a, b = (y, x) if c else (x, y)
                    ring.pa[t % PA_SLOTS, c, a, b, m * PIECE:(m + 1) * PIECE] = part[dev * PIECE:(dev + 1) * PIECE]
            ring.send0(t, LAST_ROWS)
            ring.stage_b(t, LAST_ROWS)
        if t - LAG_C < ITEMS:
            ring.stage_c(t - LAG_C, rows_of(t - LAG_C))
        d = t - LAG_D
        if d < 2 * TILES:
            store_out(d)
        else:
            total = ring.stage_d(d, LAST_ROWS)
            for m in range(4):
                dw1[:, cols((d - 2 * TILES) * 4 + m)] = total[m * PIECE:(m + 1) * PIECE]
    for t in (2 * TILES - 2, 2 * TILES - 1):
        out_copy(t).wait()


VMEM_SPEC = pl.BlockSpec(memory_space=pltpu.VMEM)
ANY_SPEC = pl.BlockSpec(memory_space=pl.ANY)
SMEM_SPEC = pl.BlockSpec(memory_space=pltpu.SMEM)
DMA = pltpu.SemaphoreType.DMA


def params(collective_id):
    return pltpu.CompilerParams(collective_id=collective_id, has_side_effects=True, vmem_limit_bytes=64_000_000)


def solution(mesh):
    sds = jax.ShapeDtypeStruct
    normed = sds((TILES, ROWS, TILE), F32)
    act = sds((ROWS, WIDTH), BF16)

    def local_step(h_a, h_b, w_one, w_two, w_three, gain_one, shift_one, gain_two, shift_two, lam_off):
        g1, b1, g2, b2 = (v.reshape(1, WIDTH) for v in (gain_one, shift_one, gain_two, shift_two))
        x1, x2, zh, inv, xh1, xh2, zn = pl.pallas_call(
            forward_kernel,
            out_shape=(act, act, act, sds((3, TILES, 2, TILE), F32), normed, normed, normed),
            in_specs=[VMEM_SPEC] * 2 + [ANY_SPEC] * 3 + [VMEM_SPEC] * 4,
            out_specs=(VMEM_SPEC,) * 4 + (ANY_SPEC,) * 3,
            scratch_shapes=[
                pltpu.VMEM((FEAT, WIDTH), BF16), pltpu.VMEM((2, TILES, WIDTH, TILE), BF16),
                pltpu.VMEM((TILES, ROWS, TILE), F32), pltpu.VMEM((3 * TILES, 8, 4, TILE), F32),
                DMA, DMA((2, TILES)), DMA((TILES,)), DMA((3 * TILES,)), DMA((3 * TILES,)),
            ],
            compiler_params=params(0), name="forward",
        )(h_a, h_b, w_one, w_two, w_three, g1, b1, g2, b2)
        dz, loss = pl.pallas_call(
            corr_kernel,
            out_shape=(act, sds((8, 128), F32)),
            in_specs=[VMEM_SPEC, ANY_SPEC, VMEM_SPEC, SMEM_SPEC],
            out_specs=(VMEM_SPEC, VMEM_SPEC),
            scratch_shapes=[
                pltpu.VMEM((TILES, ROWS, TILE), F32), pltpu.VMEM((TILES, ROWS, TILE), F32),
                pltpu.VMEM((TILES, 2, 2, 2, TILE, TILE), BF16), pltpu.VMEM((TILE, VIEW), BF16),
                pltpu.VMEM((1, TILE), F32), pltpu.VMEM((TILES + 1, 8, 4, TILE), F32),
                DMA, DMA((TILES + 1,)), DMA((TILES + 1,)),
            ] + [DMA((TILES,))] * 6 + RING_SCRATCH,
            compiler_params=params(1), name="corr",
        )(zh, zn, inv, lam_off.reshape(1, 1))
        dw, dw1, sums = pl.pallas_call(
            backward_kernel,
            out_shape=(sds((2, TILE, WIDTH), F32), sds((PIECE, WIDTH), F32), sds((4, WIDTH), F32)),
            in_specs=[VMEM_SPEC] * 5 + [ANY_SPEC] * 4 + [VMEM_SPEC] * 5,
            out_specs=(ANY_SPEC, VMEM_SPEC, VMEM_SPEC),
            scratch_shapes=[
                pltpu.VMEM((ROWS, WIDTH), BF16), pltpu.VMEM((ROWS, WIDTH), BF16),
                pltpu.VMEM((FEAT, ROWS), BF16), pltpu.VMEM((TILE, ROWS), BF16),
                pltpu.VMEM((2, TILE, WIDTH), BF16), pltpu.VMEM((4, ROWS, TILE), F32),
                pltpu.VMEM((3, ROWS, TILE), F32), pltpu.VMEM((2, TILE, TILE), F32),
                pltpu.VMEM((2 * TILES, 8, 4, TILE), F32),
                DMA((2,)), DMA((4,)), DMA((2,)), DMA((2 * TILES,)), DMA((2 * TILES,)),
            ] + RING_SCRATCH,
            compiler_params=params(2), name="backward",
        )(dz, x2, x1, h_a, h_b, w_three, w_two, xh2, xh1, inv, g1, b1, g2, b2)
        return (loss[0, 0], dw1, dw[1], dw[0], sums[3], sums[2], sums[1], sums[0])

    row_spec = P("data", None)
    whole_mat = P(None, None)
    whole_vec = P(None)
    return jax.shard_map(
        local_step, mesh=mesh,
        in_specs=(row_spec, row_spec, whole_mat, whole_mat, whole_mat,
                  whole_vec, whole_vec, whole_vec, whole_vec, P()),
        out_specs=(P(), row_spec, row_spec, row_spec, whole_vec, whole_vec, whole_vec, whole_vec),
        check_vma=False)
```

```python
import functools

import jax
import jax.numpy as jnp
from jax import lax
from jax.experimental import pallas as pl
from jax.experimental.pallas import tpu as pltpu
from jax.sharding import PartitionSpec as P

MESH = pl.DeviceIdType.MESH
F32, BF16 = jnp.float32, jnp.bfloat16
NORM_EPS = 1e-5
TOTAL_ROWS = 4096
VIEW = 512
ROWS = 2 * VIEW
FEAT = 384
WIDTH = 2048
TILE = 256
TILES = WIDTH // TILE
FWD_TILE = 512
FWD_TILES = WIDTH // FWD_TILE
PIECE = FEAT // 8
CHUNK = 128
CHUNKS = WIDTH // CHUNK
PAIRS = CHUNKS // 2
LAG_C, LAG_D, LAG_F, LAG_H, LAG_I = 1, 2, 3, 4, 5
PA_SLOTS, R0_SLOTS, R1_SLOTS, R2_SLOTS = 6, 2, 4, 4


def dot_nn(a, b):
    return jnp.dot(a, b, preferred_element_type=F32)


def dot_nt(a, b):
    return lax.dot_general(a, b, (((1,), (1,)), ((), ())), preferred_element_type=F32)


def when_in(cond, fn):
    if isinstance(cond, bool):
        if cond:
            fn()
    else:
        pl.when(cond)(fn)


def peer_of(me, r):
    out = me
    for bit in (1, 2, 4):
        if r & bit:
            out = out + bit - 2 * bit * ((me // bit) % 2)
    return out


def barrier_signal(me):
    for r in range(1, 8):
        pl.semaphore_signal(pltpu.get_barrier_semaphore(), inc=1, device_id=(peer_of(me, r),), device_id_type=MESH)


def barrier_wait():
    pl.semaphore_wait(pltpu.get_barrier_semaphore(), 7)


def cols(t, width=TILE):
    if isinstance(t, int):
        return pl.ds(t * width, width)
    return pl.ds(pl.multiple_of(t * width, width), width)


def fcols(t):
    return cols(t, FWD_TILE)


def stats_send(me, st, ssem, rsem, i):
    for r in range(1, 8):
        pltpu.make_async_remote_copy(
            src_ref=st.at[i, 0], dst_ref=st.at[i, r], send_sem=ssem.at[i], recv_sem=rsem.at[i],
            device_id=(peer_of(me, r),), device_id_type=MESH).start()


def stats_wait(st, ssem, rsem, i):
    block = st.at[i, pl.ds(1, 7)]
    pltpu.make_async_copy(block, block, rsem.at[i]).wait()
    pltpu.make_async_copy(block, block, ssem.at[i]).wait()


def stats_total(st, i):
    pairs = [st[i, 2 * k] + st[i, 2 * k + 1] for k in range(4)]
    return (pairs[0] + pairs[1]) + (pairs[2] + pairs[3])


def stats_put(st, i, values, weighted):
    for v in range(values.shape[0] // VIEW):
        part = slice(v * VIEW, (v + 1) * VIEW)
        st[i, 0, pl.ds(2 * v, 1), :] = jnp.sum(values[part], axis=0, keepdims=True)
        st[i, 0, pl.ds(2 * v + 1, 1), :] = jnp.sum(weighted[part], axis=0, keepdims=True)


def forward_kernel(h_a, h_b, w1_hbm, w2_hbm, w3_hbm, g1, b1, g2, b2,
                   inv_out, x1_hbm, x2_hbm, zh_hbm, xh1_hbm, xh2_hbm, zn_hbm,
                   x1, x2, zh, w1, wb, u, st, w1_sem, w_sem, norm_sem, act_sem, ssem, rsem):
    me = lax.axis_index("data")
    w1_copy = pltpu.make_async_copy(w1_hbm, w1, w1_sem)
    w1_copy.start()

    def w_copy(layer):
        return pltpu.make_async_copy((w2_hbm, w3_hbm)[layer], wb.at[layer], w_sem.at[layer])

    for layer in range(2):
        w_copy(layer).start()
    barrier_signal(me)
    barrier_wait()
    w1_copy.wait()

    acts = (x1, x2, zh)
    acts_hbm = (x1_hbm, x2_hbm, zh_hbm)
    normed_hbm = (xh1_hbm, xh2_hbm, zn_hbm)

    def rows_of(v):
        return pl.ds(v * VIEW, VIEW)

    def norm_copy(layer, v, q):
        return pltpu.make_async_copy(u.at[v, q], normed_hbm[layer].at[v, q], norm_sem.at[v, q])

    def act_copy(layer, v):
        return pltpu.make_async_copy(acts[layer].at[rows_of(v)], acts_hbm[layer].at[rows_of(v)], act_sem.at[layer, v])

    def slot(layer, v, q):
        return (2 * layer + v) * FWD_TILES + q

    def run(matmul=None, norm=None):
        def body(q, carry):
            if matmul is not None:
                layer, v = matmul
                if layer > 0:
                    norm_copy(layer - 1, v, q).wait()
            if norm is not None:
                n_layer, n_view = norm
                stats_wait(st, ssem, rsem, slot(n_layer, n_view, q))
            if matmul is not None:
                if layer > 0:
                    vals = dot_nn(acts[layer - 1][rows_of(v), :], wb[layer - 1, :, fcols(q)])
                else:
                    vals = dot_nn((h_a, h_b)[v][...], w1[:, fcols(q)])
            if norm is not None:
                total = stats_total(st, slot(n_layer, n_view, q)) * (1.0 / TOTAL_ROWS)
                mean = total[0:1]
                inv = lax.rsqrt(total[1:2] - mean * mean + NORM_EPS)
                inv_out[n_layer, n_view, q] = inv
                normed = (u[n_view, q] - mean) * inv
                u[n_view, q] = normed
                if n_layer < 2:
                    gain, shift = ((g1, b1), (g2, b2))[n_layer]
                    normed = jnp.maximum(gain[:, fcols(q)] * normed + shift[:, fcols(q)], 0.0)
                acts[n_layer][rows_of(n_view), fcols(q)] = normed.astype(BF16)
            if matmul is not None:
                u[v, q] = vals
                st[slot(layer, v, q), 0, pl.ds(0, 1), :] = jnp.sum(vals, axis=0, keepdims=True)
                st[slot(layer, v, q), 0, pl.ds(1, 1), :] = jnp.sum(vals * vals, axis=0, keepdims=True)
                stats_send(me, st, ssem, rsem, slot(layer, v, q))
            if norm is not None:
                norm_copy(n_layer, n_view, q).start()
            return carry

        if matmul in ((1, 0), (2, 0)):
            w_copy(matmul[0] - 1).wait()
        lax.fori_loop(0, FWD_TILES, body, 0)
        if norm is not None:
            act_copy(*norm).start()

    run(matmul=(0, 0))
    run(matmul=(0, 1))
    run(norm=(0, 0))
    run(matmul=(1, 0), norm=(0, 1))
    run(matmul=(1, 1), norm=(1, 0))
    run(matmul=(2, 0), norm=(1, 1))
    run(matmul=(2, 1), norm=(2, 0))
    run(norm=(2, 1))
    for v in range(2):
        for q in range(FWD_TILES):
            norm_copy(2, v, q).wait()
        for layer in range(3):
            act_copy(layer, v).wait()


class Ring:
    def __init__(self, me, items, pa, r0, r1, r2, sems, credits):
        self.items, self.pa, self.r0, self.r1, self.r2 = items, pa, r0, r1, r2
        self.s0, self.q0, self.s1, self.q1, self.s2, self.q2 = sems
        self.c0, self.c1, self.c2 = credits
        core = me % 2
        x, y = (me // 2) % 2, me // 4
        self.core = core
        self.f = x + core * (y - x)
        self.s = y + core * (x - y)
        x_side, y_side = me + 2 - 4 * x, me + 4 - 8 * y
        self.partner = me + 1 - 2 * core
        self.first = x_side + core * (y_side - x_side)
        self.second = y_side + core * (x_side - y_side)

    def copy(self, src, dst, send, recv, device):
        return pltpu.make_async_remote_copy(src_ref=src, dst_ref=dst, send_sem=send, recv_sem=recv,
                                            device_id=(device,), device_id_type=MESH)

    def copy0(self, t, rows):
        return self.copy(self.pa.at[t % PA_SLOTS, 1 - self.core, :, :, pl.ds(0, rows)],
                         self.r0.at[t % R0_SLOTS, :, :, pl.ds(0, rows)],
                         self.s0.at[t % R0_SLOTS], self.q0.at[t % R0_SLOTS], self.partner)

    def copy1(self, t, rows):
        return self.copy(self.pa.at[t % PA_SLOTS, self.core, 1 - self.f, :, pl.ds(0, rows)],
                         self.r1.at[t % R1_SLOTS, :, pl.ds(0, rows)],
                         self.s1.at[t % R1_SLOTS], self.q1.at[t % R1_SLOTS], self.first)

    def copy2(self, t, rows):
        return self.copy(self.pa.at[t % PA_SLOTS, self.core, self.f, 1 - self.s, pl.ds(0, rows)],
                         self.r2.at[t % R2_SLOTS, pl.ds(0, rows)],
                         self.s2.at[t % R2_SLOTS], self.q2.at[t % R2_SLOTS], self.second)

    def take_credit(self, sem, t, slots):
        when_in(t >= slots, lambda: pl.semaphore_wait(sem, 1))

    def give_credit(self, sem, t, slots, device):
        when_in(t + slots < self.items,
                lambda: pl.semaphore_signal(sem, inc=1, device_id=(device,), device_id_type=MESH))

    def send0(self, t, rows=CHUNK):
        self.take_credit(self.c0, t, R0_SLOTS)
        self.copy0(t, rows).start()

    def stage_b(self, t, rows=CHUNK):
        self.copy0(t, rows).wait()
        slot = t % PA_SLOTS
        for k in range(4):
            a, b = k // 2, k % 2
            self.pa[slot, self.core, a, b, :rows] += self.r0[t % R0_SLOTS, a, b, :rows]
        self.give_credit(self.c0, t, R0_SLOTS, self.partner)
        self.take_credit(self.c1, t, R1_SLOTS)
        self.copy1(t, rows).start()

    def stage_c(self, t, rows=CHUNK):
        self.copy1(t, rows).wait()
        slot = t % PA_SLOTS
        for b in range(2):
            self.pa[slot, self.core, self.f, b, :rows] += self.r1[t % R1_SLOTS, b, :rows]
        self.give_credit(self.c1, t, R1_SLOTS, self.first)
        self.take_credit(self.c2, t, R2_SLOTS)
        self.copy2(t, rows).start()

    def stage_d(self, t, rows=CHUNK):
        self.copy2(t, rows).wait()
        total = self.pa[t % PA_SLOTS, self.core, self.f, self.s, :rows] + self.r2[t % R2_SLOTS, :rows]
        self.give_credit(self.c2, t, R2_SLOTS, self.second)
        return total

    def partial(self, p, lt, right):
        for chip in range(4):
            part = dot_nn(lt, right[:, pl.ds(2 * chip * TILE, 2 * TILE)])
            x, y = chip % 2, chip // 2
            for c in range(2):
                a, b = (y, x) if c else (x, y)
                for k in range(2):
                    self.pa[(2 * p + k) % PA_SLOTS, c, a, b] = part[k * CHUNK:(k + 1) * CHUNK, c * TILE:(c + 1) * TILE]
        self.send0(2 * p)
        self.send0(2 * p + 1)


RING_SCRATCH = [
    pltpu.VMEM((PA_SLOTS, 2, 2, 2, CHUNK, TILE), F32),
    pltpu.VMEM((R0_SLOTS, 2, 2, CHUNK, TILE), F32),
    pltpu.VMEM((R1_SLOTS, 2, CHUNK, TILE), F32),
    pltpu.VMEM((R2_SLOTS, CHUNK, TILE), F32),
    pltpu.SemaphoreType.DMA((R0_SLOTS,)), pltpu.SemaphoreType.DMA((R0_SLOTS,)),
    pltpu.SemaphoreType.DMA((R1_SLOTS,)), pltpu.SemaphoreType.DMA((R1_SLOTS,)),
    pltpu.SemaphoreType.DMA((R2_SLOTS,)), pltpu.SemaphoreType.DMA((R2_SLOTS,)),
    pltpu.SemaphoreType.REGULAR, pltpu.SemaphoreType.REGULAR, pltpu.SemaphoreType.REGULAR,
]


LAST_COLS = 512
LAST_ITEMS = WIDTH // LAST_COLS
LAST_ROWS = LAST_COLS // TILE * PIECE
FIRST_LAST = 3 * CHUNKS
ITEMS = FIRST_LAST + LAST_ITEMS
NORM_LAG = 4
ST_LOSS = 4 * TILES


def main_kernel(zh_hbm, zn_hbm, x2_hbm, x1_hbm, h_a, h_b, w3_hbm, w2_hbm, xh2_hbm, xh1_hbm,
                inv, g1, b1, g2, b2, lam, dw3_hbm, dw2_hbm, small,
                z, normed, acc, gt, gbuf, x2, x1, du2, ht, lt, wt, stage, loss_acc, st,
                z_sem, normed_sem, x_sem, w_sem, out_sem, ssem, rsem,
                es, er, fs, fr, hs, hr, *ring_refs):
    me = lax.axis_index("data")
    z_copy = pltpu.make_async_copy(zh_hbm, z, z_sem)
    x2_copy = pltpu.make_async_copy(x2_hbm, x2, x_sem.at[0])
    x1_copy = pltpu.make_async_copy(x1_hbm, x1, x_sem.at[1])

    def normed_copies(src, sem):
        return [pltpu.make_async_copy(
            src.at[v, q // 2, :, cols(q % 2)], normed.at[q, pl.ds(v * VIEW, VIEW)], sem.at[v, q])
            for v in range(2) for q in range(TILES)]

    z_copy.start()
    barrier_signal(me)
    ring = Ring(me, ITEMS, *ring_refs[:4], ring_refs[4:10], ring_refs[10:])
    core, f, s = ring.core, ring.f, ring.s
    lam_val = lam[0, 0]
    acc[...] = jnp.zeros_like(acc)
    loss_acc[...] = jnp.zeros_like(loss_acc)
    barrier_wait()
    z_copy.wait()
    for copy in normed_copies(zn_hbm, normed_sem):
        copy.start()
    x2_copy.start()
    x1_copy.start()
    view_a, view_b = pl.ds(0, VIEW), pl.ds(VIEW, VIEW)

    def copy_e(t):
        block = gt.at[t, core, f, s]
        return ring.copy(block, block, es.at[t], er.at[t], ring.second)

    def copy_f(t):
        block = gt.at[t, core, f]
        return ring.copy(block, block, fs.at[t], fr.at[t], ring.first)

    def copy_h(t):
        block = gt.at[t, core]
        return ring.copy(block, block, hs.at[t], hr.at[t], ring.partner)

    def both(work):
        def run(p):
            work(2 * p)
            work(2 * p + 1)
        return run

    def corr_a(p):
        lt[:, view_a] = z[view_b, cols(p)].T
        ring.partial(p, lt[:, view_a], z.at[view_a])
        both(ring.stage_b)(p)

    def corr_d(t):
        corr = ring.stage_d(t) * (1.0 / TOTAL_ROWS)
        diag = (lax.broadcasted_iota(jnp.int32, corr.shape, 0) + CHUNK * t
                == lax.broadcasted_iota(jnp.int32, corr.shape, 1) + TILE * me)
        gap = 1.0 - corr
        loss_acc[...] += jnp.sum(jnp.where(diag, gap * gap, lam_val * corr * corr), axis=0, keepdims=True)
        grad = jnp.where(diag, -2.0 * gap, (2.0 * lam_val) * corr)
        gt[t, core, f, s] = (grad * (1.0 / TOTAL_ROWS)).astype(BF16)
        copy_e(t).start()

    def corr_f(t):
        copy_e(t).wait()
        copy_f(t).start()

    def corr_h(t):
        copy_f(t).wait()
        copy_h(t).start()

    def corr_i(p):
        both(lambda t: copy_h(t).wait())(p)
        for dev in range(8):
            c, x, y = dev % 2, (dev // 2) % 2, dev // 4
            a, b = (y, x) if c else (x, y)
            for k in range(2):
                gbuf[pl.ds(k * CHUNK, CHUNK), cols(dev)] = gt[2 * p + k, c, a, b]
        grad_b = dot_nt(z[view_a, :], gbuf[...])
        acc[p, view_b, :] = grad_b
        for k in range(4):
            part = dot_nn(z[view_b, cols(p)], gbuf[:, pl.ds(2 * k * TILE, 2 * TILE)])
            acc[2 * k, view_a, :] += part[:, :TILE]
            acc[2 * k + 1, view_a, :] += part[:, TILE:]
        both_views = normed_copies(zn_hbm, normed_sem)

        @pl.when(p == 0)
        def _():
            for copy in both_views:
                copy.wait()

        stats_put(st, TILES + p, grad_b, grad_b * normed[p, view_b, :])
        stats_send(me, st, ssem, rsem, TILES + p)

    def corr_tick(p, carry):
        for lag, work in ((0, corr_a), (LAG_C, both(ring.stage_c)), (LAG_D, both(corr_d)), (LAG_F, both(corr_f)),
                          (LAG_H, both(corr_h)), (LAG_I, corr_i)):
            item = p - lag
            pl.when((item >= 0) & (item < PAIRS))(functools.partial(work, item))
        return carry

    st[:, 0] = jnp.zeros((st.shape[0],) + st.shape[2:], F32)
    lax.fori_loop(0, PAIRS + LAG_I, corr_tick, 0)

    def out_sums(q, carry):
        grad = acc[q, view_a, :]
        stats_put(st, q, grad, grad * normed[q, view_a, :])
        stats_send(me, st, ssem, rsem, q)
        return carry

    lax.fori_loop(0, TILES, out_sums, 0)

    def out_norm(q, carry):
        for v in range(2):
            stats_wait(st, ssem, rsem, v * TILES + q)
            total = stats_total(st, v * TILES + q) * (1.0 / TOTAL_ROWS)
            rows = pl.ds(v * VIEW, VIEW)
            grad = acc[q, rows, :] - (total[0:1] + normed[q, rows, :] * total[1:2])
            z[rows, cols(q)] = (inv[2, v, q // 2, :, cols(q % 2)] * grad).astype(BF16)
        return carry

    out_norm(0, 0)
    x2_copy.wait()

    def out_copy(t, hbm):
        return pltpu.make_async_copy(stage.at[t % 2], hbm.at[:, cols(t % CHUNKS, CHUNK)], out_sem.at[t % 2])

    def store_out(t):
        when_in(t >= CHUNKS + 2, lambda: out_copy(t - 2, dw3_hbm).wait())
        stage[t % 2] = ring.stage_d(t).T
        if isinstance(t, int):
            out_copy(t, dw2_hbm if t >= 2 * CHUNKS else dw3_hbm).start()
        else:
            pl.when(t < 2 * CHUNKS)(lambda: out_copy(t, dw3_hbm).start())
            pl.when(t >= 2 * CHUNKS)(lambda: out_copy(t, dw2_hbm).start())

    gpre = acc
    for g in range(2):
        left, right, grad_out = ((z, x2, du2), (du2, x1, z))[g]
        w_hbm, xh_hbm = ((w3_hbm, xh2_hbm), (w2_hbm, xh1_hbm))[g]
        gain_ref, shift_ref = ((g2, b2), (g1, b1))[g]
        base = (2 + g) * TILES

        def w_copy(e, w_hbm=w_hbm):
            rows = e * TILE if isinstance(e, int) else pl.multiple_of(e * TILE, TILE)
            return pltpu.make_async_copy(w_hbm.at[pl.ds(rows, TILE), :], wt.at[e % 2], w_sem.at[e % 2])

        def grad_tile(e, left=left, w_copy=w_copy, base=base, gain_ref=gain_ref, shift_ref=shift_ref):
            w_copy(e).wait()
            grad = dot_nt(left[...], wt[e % 2])
            values = normed[e]
            pre = gain_ref[:, cols(e)] * values + shift_ref[:, cols(e)]
            grad = jnp.where(pre > 0, grad, 0.0)
            gpre[e] = grad
            stats_put(st, base + e, grad, grad * values)
            stats_send(me, st, ssem, rsem, base + e)

        def norm_tile(e, g=g, base=base, grad_out=grad_out, gain_ref=gain_ref):
            stats_wait(st, ssem, rsem, base + e)
            total = stats_total(st, base + e)
            for k in range(2):
                small[pl.ds(PIECE + 2 * g + k, 1), cols(e)] = total[k:k + 1] + total[k + 2:k + 3]
            total = total * (1.0 / TOTAL_ROWS)
            for v in range(2):
                rows = pl.ds(v * VIEW, VIEW)
                grad = gpre[e, rows, :] - (
                    total[2 * v:2 * v + 1] + normed[e, rows, :] * total[2 * v + 1:2 * v + 2])
                scale = gain_ref[:, cols(e)] * inv[1 - g, v, e // 2, :, cols(e % 2)]
                grad_out[rows, cols(e)] = (scale * grad).astype(BF16)

        def tick(q, carry, g=g, left=left, right=right, grad_tile=grad_tile, norm_tile=norm_tile, w_copy=w_copy,
                 xh_hbm=xh_hbm):
            p = (1 + g) * PAIRS + q
            lt[...] = left[:, cols(q)].T
            ring.partial(p, lt[...], right)

            @pl.when(q == 0)
            def _():
                if g == 0:
                    both(ring.stage_b)(p)
                    lax.fori_loop(1, TILES, out_norm, 0)
                w_copy(0).start()
                w_copy(1).start()
                for copy in normed_copies(xh_hbm, normed_sem):
                    copy.start()

            @pl.when(q == 1)
            def _():
                for copy in normed_copies(xh_hbm, normed_sem):
                    copy.wait()

            def step(k, carry):
                e = 2 * (q - 1) + k
                pl.when(e < TILES)(lambda: grad_tile(e))
                pl.when((e >= NORM_LAG) & (e < TILES + NORM_LAG))(lambda: norm_tile(e - NORM_LAG))
                pl.when(e + 2 < TILES)(lambda: w_copy(e + 2).start())
                return carry

            @pl.when(q >= 1)
            def _():
                lax.fori_loop(0, 2, step, 0)

            if g == 0:
                pl.when(q > 0)(lambda: both(ring.stage_b)(p))
                pl.when(q >= LAG_C)(lambda: both(ring.stage_c)(p - LAG_C))
                pl.when(q >= LAG_D)(lambda: both(store_out)(p - LAG_D))
            else:
                both(ring.stage_b)(p)
                both(ring.stage_c)(p - LAG_C)
                both(store_out)(p - LAG_D)
            return carry

        if g == 1:
            x1_copy.wait()
        lax.fori_loop(0, PAIRS, tick, 0)

    ht[:, view_a] = h_a[...].T
    ht[:, view_b] = h_b[...].T
    per_item = LAST_COLS // TILE

    def rows_of(t):
        return LAST_ROWS if t >= FIRST_LAST else CHUNK

    for t in range(FIRST_LAST, ITEMS + 2 * LAG_D):
        if t < ITEMS:
            for m in range(per_item):
                part = dot_nn(ht[...], z[:, cols((t - FIRST_LAST) * per_item + m)])
                for dev in range(8):
                    c, x, y = dev % 2, (dev // 2) % 2, dev // 4
                    a, b = (y, x) if c else (x, y)
                    ring.pa[t % PA_SLOTS, c, a, b, m * PIECE:(m + 1) * PIECE] = part[dev * PIECE:(dev + 1) * PIECE]
            ring.send0(t, LAST_ROWS)
            ring.stage_b(t, LAST_ROWS)
        if t - 2 * LAG_C < ITEMS:
            ring.stage_c(t - 2 * LAG_C, rows_of(t - 2 * LAG_C))
        d = t - 2 * LAG_D
        if d < FIRST_LAST:
            store_out(d)
        else:
            total = ring.stage_d(d, LAST_ROWS)
            for m in range(per_item):
                small[pl.ds(0, PIECE), cols((d - FIRST_LAST) * per_item + m)] = total[m * PIECE:(m + 1) * PIECE]
        if t == FIRST_LAST:
            st[ST_LOSS, 0, pl.ds(0, 1), :] = loss_acc[...]
            stats_send(me, st, ssem, rsem, ST_LOSS)
    for t in (FIRST_LAST - 2, FIRST_LAST - 1):
        out_copy(t, dw2_hbm).wait()
    stats_wait(st, ssem, rsem, ST_LOSS)
    loss = jnp.sum(stats_total(st, ST_LOSS), keepdims=True)
    small[pl.ds(PIECE + 4, 4), :] = jnp.broadcast_to(loss, (4, WIDTH))


def finish_kernel(dw3_in, dw2_in, small_in, dw1, dw2, dw3, gg1, gs1, gg2, gs2, loss, v3, v2, vs, in_sem, out_sem):
    loads = [pltpu.make_async_copy(small_in, vs, in_sem.at[0])]
    stores = [pltpu.make_async_copy(vs.at[pl.ds(0, PIECE)], dw1, out_sem.at[0])]
    for k, (src, mid, dst) in enumerate(((dw3_in, v3, dw3), (dw2_in, v2, dw2))):
        for part in range(4):
            rows = pl.ds(part * TILE // 4, TILE // 4)
            i = 1 + 4 * k + part
            loads.append(pltpu.make_async_copy(src.at[rows], mid.at[rows], in_sem.at[i]))
            stores.append(pltpu.make_async_copy(mid.at[rows], dst.at[rows], out_sem.at[i]))
    for load in loads:
        load.start()
    for load, store in zip(loads, stores):
        load.wait()
        store.start()
    for k, ref in enumerate((gs2, gg2, gs1, gg1)):
        ref[...] = vs[pl.ds(PIECE + k, 1), :]
    loss[...] = vs[pl.ds(PIECE + 4, 1), pl.ds(0, 1)]
    for store in stores:
        store.wait()


VMEM_SPEC = pl.BlockSpec(memory_space=pltpu.VMEM)
ANY_SPEC = pl.BlockSpec(memory_space=pl.ANY)
SMEM_SPEC = pl.BlockSpec(memory_space=pltpu.SMEM)
DMA = pltpu.SemaphoreType.DMA


def params(collective_id):
    return pltpu.CompilerParams(collective_id=collective_id, has_side_effects=True, vmem_limit_bytes=64_000_000)


def solution(mesh):
    sds = jax.ShapeDtypeStruct
    normed = sds((2, FWD_TILES, VIEW, FWD_TILE), F32)
    act = sds((ROWS, WIDTH), BF16)
    weight = sds((TILE, WIDTH), F32)
    vector = sds((1, WIDTH), F32)
    small = 2 * PIECE - 40

    def local_step(h_a, h_b, w_one, w_two, w_three, gain_one, shift_one, gain_two, shift_two, lam_off):
        g1, b1, g2, b2 = (v.reshape(1, WIDTH) for v in (gain_one, shift_one, gain_two, shift_two))
        inv, x1, x2, zh, xh1, xh2, zn = pl.pallas_call(
            forward_kernel,
            out_shape=(sds((3, 2, FWD_TILES, 1, FWD_TILE), F32), act, act, act, normed, normed, normed),
            in_specs=[VMEM_SPEC] * 2 + [ANY_SPEC] * 3 + [VMEM_SPEC] * 4,
            out_specs=(VMEM_SPEC,) + (ANY_SPEC,) * 6,
            scratch_shapes=[
                pltpu.VMEM((ROWS, WIDTH), BF16), pltpu.VMEM((ROWS, WIDTH), BF16), pltpu.VMEM((ROWS, WIDTH), BF16),
                pltpu.VMEM((FEAT, WIDTH), BF16), pltpu.VMEM((2, WIDTH, WIDTH), BF16),
                pltpu.VMEM((2, FWD_TILES, VIEW, FWD_TILE), F32), pltpu.VMEM((6 * FWD_TILES, 8, 2, FWD_TILE), F32),
                DMA, DMA((2,)), DMA((2, FWD_TILES)), DMA((3, 2)), DMA((6 * FWD_TILES,)), DMA((6 * FWD_TILES,)),
            ],
            compiler_params=params(0), name="forward",
        )(h_a, h_b, w_one, w_two, w_three, g1, b1, g2, b2)
        dw3, dw2, rest = pl.pallas_call(
            main_kernel,
            out_shape=(weight, weight, sds((small, WIDTH), F32)),
            in_specs=[ANY_SPEC] * 4 + [VMEM_SPEC] * 2 + [ANY_SPEC] * 4 + [VMEM_SPEC] * 5 + [SMEM_SPEC],
            out_specs=(ANY_SPEC, ANY_SPEC, VMEM_SPEC),
            scratch_shapes=[
                pltpu.VMEM((ROWS, WIDTH), BF16), pltpu.VMEM((TILES, ROWS, TILE), F32),
                pltpu.VMEM((TILES, ROWS, TILE), F32), pltpu.VMEM((CHUNKS, 2, 2, 2, CHUNK, TILE), BF16),
                pltpu.VMEM((TILE, WIDTH), BF16),
                pltpu.VMEM((ROWS, WIDTH), BF16), pltpu.VMEM((ROWS, WIDTH), BF16), pltpu.VMEM((ROWS, WIDTH), BF16),
                pltpu.VMEM((FEAT, ROWS), BF16), pltpu.VMEM((TILE, ROWS), BF16),
                pltpu.VMEM((2, TILE, WIDTH), BF16), pltpu.VMEM((2, TILE, CHUNK), F32),
                pltpu.VMEM((1, TILE), F32), pltpu.VMEM((ST_LOSS + 1, 8, 4, TILE), F32),
                DMA, DMA((2, TILES)), DMA((2,)), DMA((2,)), DMA((2,)), DMA((ST_LOSS + 1,)), DMA((ST_LOSS + 1,)),
            ] + [DMA((CHUNKS,))] * 6 + RING_SCRATCH,
            compiler_params=params(1), name="main",
        )(zh, zn, x2, x1, h_a, h_b, w_three, w_two, xh2, xh1, inv, g1, b1, g2, b2, lam_off.reshape(1, 1))
        dw1, dw2, dw3, gg1, gs1, gg2, gs2, loss = pl.pallas_call(
            finish_kernel,
            out_shape=(sds((PIECE, WIDTH), F32), weight, weight, vector, vector, vector, vector, sds((1, 1), F32)),
            in_specs=[ANY_SPEC] * 3,
            out_specs=(ANY_SPEC,) * 3 + (VMEM_SPEC,) * 5,
            scratch_shapes=[
                pltpu.VMEM((TILE, WIDTH), F32), pltpu.VMEM((TILE, WIDTH), F32), pltpu.VMEM((small, WIDTH), F32),
                DMA((9,)), DMA((9,)),
            ],
            compiler_params=pltpu.CompilerParams(vmem_limit_bytes=66_000_000), name="finish",
        )(dw3, dw2, rest)
        return (loss.reshape(()), dw1, dw2, dw3, gg1.reshape(WIDTH), gs1.reshape(WIDTH),
                gg2.reshape(WIDTH), gs2.reshape(WIDTH))

    row_spec = P("data", None)
    whole_mat = P(None, None)
    whole_vec = P(None)
    return jax.shard_map(
        local_step, mesh=mesh,
        in_specs=(row_spec, row_spec, whole_mat, whole_mat, whole_mat,
                  whole_vec, whole_vec, whole_vec, whole_vec, P()),
        out_specs=(P(), row_spec, row_spec, row_spec, whole_vec, whole_vec, whole_vec, whole_vec),
        check_vma=False)
```

```python
import functools

import jax
import jax.numpy as jnp
from jax import lax
from jax.experimental import pallas as pl
from jax.experimental.pallas import tpu as pltpu
from jax.sharding import PartitionSpec as P

MESH = pl.DeviceIdType.MESH
F32, BF16 = jnp.float32, jnp.bfloat16
NORM_EPS = 1e-5
TOTAL_ROWS = 4096
VIEW = 512
ROWS = 2 * VIEW
FEAT = 384
WIDTH = 2048
TILE = 256
TILES = WIDTH // TILE
FWD_TILE = 512
FWD_TILES = WIDTH // FWD_TILE
PIECE = FEAT // 8
CHUNK = 128
CHUNKS = WIDTH // CHUNK
PAIRS = CHUNKS // 2
LAG_C, LAG_D, LAG_F, LAG_H, LAG_I = 1, 2, 3, 4, 5
PA_SLOTS, R0_SLOTS, R1_SLOTS, R2_SLOTS = 6, 2, 4, 4


def dot_nn(a, b):
    return jnp.dot(a, b, preferred_element_type=F32)


def dot_nt(a, b):
    return lax.dot_general(a, b, (((1,), (1,)), ((), ())), preferred_element_type=F32)


def when_in(cond, fn):
    if isinstance(cond, bool):
        if cond:
            fn()
    else:
        pl.when(cond)(fn)


def peer_of(me, r):
    out = me
    for bit in (1, 2, 4):
        if r & bit:
            out = out + bit - 2 * bit * ((me // bit) % 2)
    return out


def barrier_signal(me):
    for r in range(1, 8):
        pl.semaphore_signal(pltpu.get_barrier_semaphore(), inc=1, device_id=(peer_of(me, r),), device_id_type=MESH)


def barrier_wait():
    pl.semaphore_wait(pltpu.get_barrier_semaphore(), 7)


def cols(t, width=TILE):
    if isinstance(t, int):
        return pl.ds(t * width, width)
    return pl.ds(pl.multiple_of(t * width, width), width)


def fcols(t):
    return cols(t, FWD_TILE)


def stats_send(me, st, ssem, rsem, i):
    for r in range(1, 8):
        pltpu.make_async_remote_copy(
            src_ref=st.at[i, 0], dst_ref=st.at[i, r], send_sem=ssem.at[i], recv_sem=rsem.at[i],
            device_id=(peer_of(me, r),), device_id_type=MESH).start()


def stats_wait(st, ssem, rsem, i):
    block = st.at[i, pl.ds(1, 7)]
    pltpu.make_async_copy(block, block, rsem.at[i]).wait()
    pltpu.make_async_copy(block, block, ssem.at[i]).wait()


def stats_total(st, i):
    pairs = [st[i, 2 * k] + st[i, 2 * k + 1] for k in range(4)]
    return (pairs[0] + pairs[1]) + (pairs[2] + pairs[3])


def stats_put(st, i, values, weighted):
    for v in range(values.shape[0] // VIEW):
        part = slice(v * VIEW, (v + 1) * VIEW)
        st[i, 0, pl.ds(2 * v, 1), :] = jnp.sum(values[part], axis=0, keepdims=True)
        st[i, 0, pl.ds(2 * v + 1, 1), :] = jnp.sum(weighted[part], axis=0, keepdims=True)


def copies_in(hbm, vmem, sem):
    return [pltpu.make_async_copy(src, dst, sem.at[i]) for i, (src, dst) in enumerate(zip(hbm, vmem))]


def forward_kernel(ha_hbm, hb_hbm, w1_hbm, w2_hbm, w3_hbm, g1_hbm, b1_hbm, g2_hbm, b2_hbm,
                   inv_out, x1_hbm, x2_hbm, zh_hbm, xh1_hbm, xh2_hbm, zn_hbm,
                   x1, x2, zh, w1, wb, u, st, h_a, h_b, g1, b1, g2, b2,
                   w1_sem, w_sem, norm_sem, act_sem, ssem, rsem, in_sem):
    me = lax.axis_index("data")
    inputs = copies_in((ha_hbm, hb_hbm, g1_hbm, b1_hbm, g2_hbm, b2_hbm), (h_a, h_b, g1, b1, g2, b2), in_sem)
    w1_copy = pltpu.make_async_copy(w1_hbm, w1, w1_sem)
    w1_copy.start()
    for copy in inputs:
        copy.start()

    def w_copy(layer):
        return pltpu.make_async_copy((w2_hbm, w3_hbm)[layer], wb.at[layer], w_sem.at[layer])

    barrier_signal(me)
    w1_copy.wait()
    for copy in inputs:
        copy.wait()
    for layer in range(2):
        w_copy(layer).start()

    acts = (x1, x2, zh)
    acts_hbm = (x1_hbm, x2_hbm, zh_hbm)
    normed_hbm = (xh1_hbm, xh2_hbm, zn_hbm)

    def rows_of(v):
        return pl.ds(v * VIEW, VIEW)

    def norm_copy(layer, v, q):
        return pltpu.make_async_copy(u.at[v, q], normed_hbm[layer].at[v, q], norm_sem.at[v, q])

    def act_copy(layer, v, q):
        return pltpu.make_async_copy(acts[layer].at[rows_of(v), fcols(q)], acts_hbm[layer].at[rows_of(v), fcols(q)],
                                     act_sem.at[layer, v, q])

    def slot(layer, v, q):
        return (2 * layer + v) * FWD_TILES + q

    def run(matmul=None, norm=None):
        def body(q, carry):
            if matmul is not None:
                layer, v = matmul
                if layer > 0:
                    norm_copy(layer - 1, v, q).wait()
            if norm is not None:
                n_layer, n_view = norm
                stats_wait(st, ssem, rsem, slot(n_layer, n_view, q))
            if matmul is not None:
                if layer > 0:
                    vals = dot_nn(acts[layer - 1][rows_of(v), :], wb[layer - 1, :, fcols(q)])
                else:
                    vals = dot_nn((h_a, h_b)[v][...], w1[:, fcols(q)])
            if norm is not None:
                total = stats_total(st, slot(n_layer, n_view, q)) * (1.0 / TOTAL_ROWS)
                mean = total[0:1]
                inv = lax.rsqrt(total[1:2] - mean * mean + NORM_EPS)
                inv_out[n_layer, n_view, q] = inv
                normed = (u[n_view, q] - mean) * inv
                u[n_view, q] = normed
                if n_layer < 2:
                    gain, shift = ((g1, b1), (g2, b2))[n_layer]
                    normed = jnp.maximum(gain[:, fcols(q)] * normed + shift[:, fcols(q)], 0.0)
                acts[n_layer][rows_of(n_view), fcols(q)] = normed.astype(BF16)
            if matmul is not None:
                u[v, q] = vals
                st[slot(layer, v, q), 0, pl.ds(0, 1), :] = jnp.sum(vals, axis=0, keepdims=True)
                st[slot(layer, v, q), 0, pl.ds(1, 1), :] = jnp.sum(vals * vals, axis=0, keepdims=True)
                if matmul != (0, 0):
                    stats_send(me, st, ssem, rsem, slot(layer, v, q))
            if norm is not None:
                act_copy(n_layer, n_view, q).start()
                norm_copy(n_layer, n_view, q).start()
            return carry

        if matmul in ((1, 0), (2, 0)):
            w_copy(matmul[0] - 1).wait()
        lax.fori_loop(0, FWD_TILES, body, 0)

    run(matmul=(0, 0))
    barrier_wait()
    for q in range(FWD_TILES):
        stats_send(me, st, ssem, rsem, slot(0, 0, q))
    run(matmul=(0, 1))
    run(norm=(0, 0))
    run(matmul=(1, 0), norm=(0, 1))
    run(matmul=(1, 1), norm=(1, 0))
    run(matmul=(2, 0), norm=(1, 1))
    run(matmul=(2, 1), norm=(2, 0))
    run(norm=(2, 1))
    for v in range(2):
        for q in range(FWD_TILES):
            norm_copy(2, v, q).wait()
            for layer in range(3):
                act_copy(layer, v, q).wait()


class Ring:
    def __init__(self, me, items, pa, r0, r1, r2, sems, credits):
        self.items, self.pa, self.r0, self.r1, self.r2 = items, pa, r0, r1, r2
        self.s0, self.q0, self.s1, self.q1, self.s2, self.q2 = sems
        self.c0, self.c1, self.c2 = credits
        core = me % 2
        x, y = (me // 2) % 2, me // 4
        self.core = core
        self.f = x + core * (y - x)
        self.s = y + core * (x - y)
        x_side, y_side = me + 2 - 4 * x, me + 4 - 8 * y
        self.partner = me + 1 - 2 * core
        self.first = x_side + core * (y_side - x_side)
        self.second = y_side + core * (x_side - y_side)

    def copy(self, src, dst, send, recv, device):
        return pltpu.make_async_remote_copy(src_ref=src, dst_ref=dst, send_sem=send, recv_sem=recv,
                                            device_id=(device,), device_id_type=MESH)

    def copy0(self, t, rows):
        return self.copy(self.pa.at[t % PA_SLOTS, 1 - self.core, :, :, pl.ds(0, rows)],
                         self.r0.at[t % R0_SLOTS, :, :, pl.ds(0, rows)],
                         self.s0.at[t % R0_SLOTS], self.q0.at[t % R0_SLOTS], self.partner)

    def copy1(self, t, rows):
        return self.copy(self.pa.at[t % PA_SLOTS, self.core, 1 - self.f, :, pl.ds(0, rows)],
                         self.r1.at[t % R1_SLOTS, :, pl.ds(0, rows)],
                         self.s1.at[t % R1_SLOTS], self.q1.at[t % R1_SLOTS], self.first)

    def copy2(self, t, rows):
        return self.copy(self.pa.at[t % PA_SLOTS, self.core, self.f, 1 - self.s, pl.ds(0, rows)],
                         self.r2.at[t % R2_SLOTS, pl.ds(0, rows)],
                         self.s2.at[t % R2_SLOTS], self.q2.at[t % R2_SLOTS], self.second)

    def take_credit(self, sem, t, slots):
        when_in(t >= slots, lambda: pl.semaphore_wait(sem, 1))

    def give_credit(self, sem, t, slots, device):
        when_in(t + slots < self.items,
                lambda: pl.semaphore_signal(sem, inc=1, device_id=(device,), device_id_type=MESH))

    def send0(self, t, rows=CHUNK):
        self.take_credit(self.c0, t, R0_SLOTS)
        self.copy0(t, rows).start()

    def stage_b(self, t, rows=CHUNK):
        self.copy0(t, rows).wait()
        slot = t % PA_SLOTS
        for k in range(4):
            a, b = k // 2, k % 2
            self.pa[slot, self.core, a, b, :rows] += self.r0[t % R0_SLOTS, a, b, :rows]
        self.give_credit(self.c0, t, R0_SLOTS, self.partner)
        self.take_credit(self.c1, t, R1_SLOTS)
        self.copy1(t, rows).start()

    def stage_c(self, t, rows=CHUNK):
        self.copy1(t, rows).wait()
        slot = t % PA_SLOTS
        for b in range(2):
            self.pa[slot, self.core, self.f, b, :rows] += self.r1[t % R1_SLOTS, b, :rows]
        self.give_credit(self.c1, t, R1_SLOTS, self.first)
        self.take_credit(self.c2, t, R2_SLOTS)
        self.copy2(t, rows).start()

    def stage_d(self, t, rows=CHUNK):
        self.copy2(t, rows).wait()
        total = self.pa[t % PA_SLOTS, self.core, self.f, self.s, :rows] + self.r2[t % R2_SLOTS, :rows]
        self.give_credit(self.c2, t, R2_SLOTS, self.second)
        return total

    def partial(self, p, lt, right):
        for chip in range(4):
            part = dot_nn(lt, right[:, pl.ds(2 * chip * TILE, 2 * TILE)])
            x, y = chip % 2, chip // 2
            for c in range(2):
                a, b = (y, x) if c else (x, y)
                for k in range(2):
                    self.pa[(2 * p + k) % PA_SLOTS, c, a, b] = part[k * CHUNK:(k + 1) * CHUNK, c * TILE:(c + 1) * TILE]
        self.send0(2 * p)
        self.send0(2 * p + 1)


RING_SCRATCH = [
    pltpu.VMEM((PA_SLOTS, 2, 2, 2, CHUNK, TILE), F32),
    pltpu.VMEM((R0_SLOTS, 2, 2, CHUNK, TILE), F32),
    pltpu.VMEM((R1_SLOTS, 2, CHUNK, TILE), F32),
    pltpu.VMEM((R2_SLOTS, CHUNK, TILE), F32),
    pltpu.SemaphoreType.DMA((R0_SLOTS,)), pltpu.SemaphoreType.DMA((R0_SLOTS,)),
    pltpu.SemaphoreType.DMA((R1_SLOTS,)), pltpu.SemaphoreType.DMA((R1_SLOTS,)),
    pltpu.SemaphoreType.DMA((R2_SLOTS,)), pltpu.SemaphoreType.DMA((R2_SLOTS,)),
    pltpu.SemaphoreType.REGULAR, pltpu.SemaphoreType.REGULAR, pltpu.SemaphoreType.REGULAR,
]


LAST_COLS = 512
LAST_ITEMS = WIDTH // LAST_COLS
LAST_ROWS = LAST_COLS // TILE * PIECE
FIRST_LAST = 3 * CHUNKS
ITEMS = FIRST_LAST + LAST_ITEMS
NORM_LAG = 2
ST_LOSS = 4 * TILES


def main_kernel(zh_hbm, zn_hbm, x2_hbm, x1_hbm, ha_hbm, hb_hbm, w3_hbm, w2_hbm, xh2_hbm, xh1_hbm,
                inv_hbm, g1_hbm, b1_hbm, g2_hbm, b2_hbm, lam, dw3_hbm, dw2_hbm, small,
                z, normed, acc, gt, gbuf, x2, x1, du2, ht, lt, wt, stage, loss_acc, st,
                h_a, h_b, g1, b1, g2, b2, inv, in_sem,
                z_sem, normed_sem, x_sem, w_sem, out_sem, ssem, rsem,
                es, er, fs, fr, hs, hr, *ring_refs):
    me = lax.axis_index("data")
    z_copy = pltpu.make_async_copy(zh_hbm, z, z_sem)
    x2_copy = pltpu.make_async_copy(x2_hbm, x2, x_sem.at[0])
    x1_copy = pltpu.make_async_copy(x1_hbm, x1, x_sem.at[1])

    def normed_copies(src, sem):
        return [pltpu.make_async_copy(
            src.at[v, q // 2, :, cols(q % 2)], normed.at[q, pl.ds(v * VIEW, VIEW)], sem.at[v, q])
            for v in range(2) for q in range(TILES)]

    z_copy.start()
    barrier_signal(me)
    ring = Ring(me, ITEMS, *ring_refs[:4], ring_refs[4:10], ring_refs[10:])
    core, f, s = ring.core, ring.f, ring.s
    lam_val = lam[0, 0]
    acc[...] = jnp.zeros_like(acc)
    loss_acc[...] = jnp.zeros_like(loss_acc)
    barrier_wait()
    z_copy.wait()
    for copy in normed_copies(zn_hbm, normed_sem):
        copy.start()
    inputs = copies_in((ha_hbm, hb_hbm, g1_hbm, b1_hbm, g2_hbm, b2_hbm, inv_hbm),
                       (h_a, h_b, g1, b1, g2, b2, inv), in_sem)
    for copy in inputs:
        copy.start()
    x2_copy.start()
    x1_copy.start()
    view_a, view_b = pl.ds(0, VIEW), pl.ds(VIEW, VIEW)

    def copy_e(t):
        block = gt.at[t, core, f, s]
        return ring.copy(block, block, es.at[t], er.at[t], ring.second)

    def copy_f(t):
        block = gt.at[t, core, f]
        return ring.copy(block, block, fs.at[t], fr.at[t], ring.first)

    def copy_h(t):
        block = gt.at[t, core]
        return ring.copy(block, block, hs.at[t], hr.at[t], ring.partner)

    def both(work):
        def run(p):
            work(2 * p)
            work(2 * p + 1)
        return run

    def corr_a(p):
        lt[:, view_a] = z[view_b, cols(p)].T
        ring.partial(p, lt[:, view_a], z.at[view_a])
        both(ring.stage_b)(p)

    def corr_d(t):
        corr = ring.stage_d(t) * (1.0 / TOTAL_ROWS)
        diag = (lax.broadcasted_iota(jnp.int32, corr.shape, 0) + CHUNK * t
                == lax.broadcasted_iota(jnp.int32, corr.shape, 1) + TILE * me)
        gap = 1.0 - corr
        loss_acc[...] += jnp.sum(jnp.where(diag, gap * gap, lam_val * corr * corr), axis=0, keepdims=True)
        grad = jnp.where(diag, -2.0 * gap, (2.0 * lam_val) * corr)
        gt[t, core, f, s] = (grad * (1.0 / TOTAL_ROWS)).astype(BF16)
        copy_e(t).start()

    def corr_f(t):
        copy_e(t).wait()
        copy_f(t).start()

    def corr_h(t):
        copy_f(t).wait()
        copy_h(t).start()

    def corr_i(p):
        both(lambda t: copy_h(t).wait())(p)
        for dev in range(8):
            c, x, y = dev % 2, (dev // 2) % 2, dev // 4
            a, b = (y, x) if c else (x, y)
            for k in range(2):
                gbuf[pl.ds(k * CHUNK, CHUNK), cols(dev)] = gt[2 * p + k, c, a, b]
        grad_b = dot_nt(z[view_a, :], gbuf[...])
        acc[p, view_b, :] = grad_b
        for k in range(4):
            part = dot_nn(z[view_b, cols(p)], gbuf[:, pl.ds(2 * k * TILE, 2 * TILE)])
            acc[2 * k, view_a, :] += part[:, :TILE]
            acc[2 * k + 1, view_a, :] += part[:, TILE:]
        both_views = normed_copies(zn_hbm, normed_sem)

        @pl.when(p == 0)
        def _():
            for copy in both_views:
                copy.wait()

        stats_put(st, TILES + p, grad_b, grad_b * normed[p, view_b, :])
        stats_send(me, st, ssem, rsem, TILES + p)

    def corr_tick(p, carry):
        last = PAIRS - 1
        for lag, work, end in ((0, corr_a, last), (LAG_C, both(ring.stage_c), last), (LAG_D, both(corr_d), last),
                               (LAG_F, both(corr_f), last), (LAG_I, corr_i, last - 2),
                               (LAG_H, both(corr_h), last), (LAG_I, corr_i, last)):
            item = p - lag
            start = 0 if (lag, end) != (LAG_I, last) else last - 1
            pl.when((item >= start) & (item <= end))(functools.partial(work, item))
        return carry

    st[:, 0] = jnp.zeros((st.shape[0],) + st.shape[2:], F32)
    lax.fori_loop(0, PAIRS + LAG_I, corr_tick, 0)

    def out_sums(q, carry):
        grad = acc[q, view_a, :]
        stats_put(st, q, grad, grad * normed[q, view_a, :])
        stats_send(me, st, ssem, rsem, q)
        return carry

    lax.fori_loop(0, TILES, out_sums, 0)

    def out_norm(q, carry):
        for v in range(2):
            stats_wait(st, ssem, rsem, v * TILES + q)
            total = stats_total(st, v * TILES + q) * (1.0 / TOTAL_ROWS)
            rows = pl.ds(v * VIEW, VIEW)
            grad = acc[q, rows, :] - (total[0:1] + normed[q, rows, :] * total[1:2])
            z[rows, cols(q)] = (inv[2, v, q // 2, :, cols(q % 2)] * grad).astype(BF16)
        return carry

    for copy in inputs:
        copy.wait()
    out_norm(0, 0)
    x2_copy.wait()

    def out_copy(t, hbm):
        return pltpu.make_async_copy(stage.at[t % 2], hbm.at[:, cols(t % CHUNKS, CHUNK)], out_sem.at[t % 2])

    def store_out(t):
        when_in(t >= CHUNKS + 2, lambda: out_copy(t - 2, dw3_hbm).wait())
        stage[t % 2] = ring.stage_d(t).T
        if isinstance(t, int):
            out_copy(t, dw2_hbm if t >= 2 * CHUNKS else dw3_hbm).start()
        else:
            pl.when(t < 2 * CHUNKS)(lambda: out_copy(t, dw3_hbm).start())
            pl.when(t >= 2 * CHUNKS)(lambda: out_copy(t, dw2_hbm).start())

    gpre = acc
    for g in range(2):
        left, right, grad_out = ((z, x2, du2), (du2, x1, z))[g]
        w_hbm, xh_hbm = ((w3_hbm, xh2_hbm), (w2_hbm, xh1_hbm))[g]
        gain_ref, shift_ref = ((g2, b2), (g1, b1))[g]
        base = (2 + g) * TILES

        def w_copy(e, w_hbm=w_hbm):
            rows = e * TILE if isinstance(e, int) else pl.multiple_of(e * TILE, TILE)
            return pltpu.make_async_copy(w_hbm.at[pl.ds(rows, TILE), :], wt.at[e % 2], w_sem.at[e % 2])

        def grad_step(e, grad, norm, g=g, left=left, w_copy=w_copy, base=base, grad_out=grad_out,
                      gain_ref=gain_ref, shift_ref=shift_ref):
            d = e - NORM_LAG
            if grad:
                w_copy(e).wait()
            if norm:
                stats_wait(st, ssem, rsem, base + d)
            if grad:
                vals = dot_nt(left[...], wt[e % 2])
            if norm:
                total = stats_total(st, base + d)
                for k in range(2):
                    small[pl.ds(PIECE + 2 * g + k, 1), cols(d)] = total[k:k + 1] + total[k + 2:k + 3]
                total = total * (1.0 / TOTAL_ROWS)
                for v in range(2):
                    rows = pl.ds(v * VIEW, VIEW)
                    out = gpre[d, rows, :] - (
                        total[2 * v:2 * v + 1] + normed[d, rows, :] * total[2 * v + 1:2 * v + 2])
                    scale = gain_ref[:, cols(d)] * inv[1 - g, v, d // 2, :, cols(d % 2)]
                    grad_out[rows, cols(d)] = (scale * out).astype(BF16)
            if grad:
                values = normed[e]
                pre = gain_ref[:, cols(e)] * values + shift_ref[:, cols(e)]
                vals = jnp.where(pre > 0, vals, 0.0)
                gpre[e] = vals
                stats_put(st, base + e, vals, vals * values)
                stats_send(me, st, ssem, rsem, base + e)
                pl.when(e + 2 < TILES)(lambda: w_copy(e + 2).start())

        def tick(q, carry, g=g, left=left, right=right, grad_step=grad_step, w_copy=w_copy,
                 xh_hbm=xh_hbm):
            p = (1 + g) * PAIRS + q
            lt[...] = left[:, cols(q)].T
            ring.partial(p, lt[...], right)

            @pl.when(q == 0)
            def _():
                if g == 0:
                    both(ring.stage_b)(p)
                    lax.fori_loop(1, TILES, out_norm, 0)
                w_copy(0).start()
                w_copy(1).start()
                for copy in normed_copies(xh_hbm, normed_sem):
                    copy.start()

            @pl.when(q == 1)
            def _():
                for copy in normed_copies(xh_hbm, normed_sem):
                    copy.wait()

            def step(e, carry):
                pl.when(e < NORM_LAG)(lambda: grad_step(e, True, False))
                pl.when((e >= NORM_LAG) & (e < TILES))(lambda: grad_step(e, True, True))
                pl.when(e >= TILES)(lambda: grad_step(e, False, True))
                return carry

            @pl.when(q >= 1)
            def _():
                lax.fori_loop((q - 1) * 3 // 2, q * 3 // 2, step, 0)

            if g == 0:
                pl.when(q > 0)(lambda: both(ring.stage_b)(p))
                pl.when(q >= LAG_C)(lambda: both(ring.stage_c)(p - LAG_C))
                pl.when(q >= LAG_D)(lambda: both(store_out)(p - LAG_D))
            else:
                both(ring.stage_b)(p)
                both(ring.stage_c)(p - LAG_C)
                both(store_out)(p - LAG_D)
            return carry

        if g == 1:
            x1_copy.wait()
        lax.fori_loop(0, PAIRS, tick, 0)

    ht[:, view_a] = h_a[...].T
    ht[:, view_b] = h_b[...].T
    per_item = LAST_COLS // TILE

    def rows_of(t):
        return LAST_ROWS if t >= FIRST_LAST else CHUNK

    for t in range(FIRST_LAST, ITEMS + 2 * LAG_D):
        if t < ITEMS:
            for m in range(per_item):
                part = dot_nn(ht[...], z[:, cols((t - FIRST_LAST) * per_item + m)])
                for dev in range(8):
                    c, x, y = dev % 2, (dev // 2) % 2, dev // 4
                    a, b = (y, x) if c else (x, y)
                    ring.pa[t % PA_SLOTS, c, a, b, m * PIECE:(m + 1) * PIECE] = part[dev * PIECE:(dev + 1) * PIECE]
            ring.send0(t, LAST_ROWS)
            ring.stage_b(t, LAST_ROWS)
        if t - 2 * LAG_C < ITEMS:
            ring.stage_c(t - 2 * LAG_C, rows_of(t - 2 * LAG_C))
        d = t - 2 * LAG_D
        if d < FIRST_LAST:
            store_out(d)
        else:
            total = ring.stage_d(d, LAST_ROWS)
            for m in range(per_item):
                small[pl.ds(0, PIECE), cols((d - FIRST_LAST) * per_item + m)] = total[m * PIECE:(m + 1) * PIECE]
        if t == FIRST_LAST:
            st[ST_LOSS, 0, pl.ds(0, 1), :] = loss_acc[...]
            stats_send(me, st, ssem, rsem, ST_LOSS)
    for t in (FIRST_LAST - 2, FIRST_LAST - 1):
        out_copy(t, dw2_hbm).wait()
    stats_wait(st, ssem, rsem, ST_LOSS)
    loss = jnp.sum(stats_total(st, ST_LOSS), keepdims=True)
    small[pl.ds(PIECE + 4, 4), :] = jnp.broadcast_to(loss, (4, WIDTH))


def finish_kernel(dw3_in, dw2_in, small_in, dw1, dw2, dw3, gg1, gs1, gg2, gs2, loss, v3, v2, vs, in_sem, out_sem):
    loads = [pltpu.make_async_copy(small_in, vs, in_sem.at[0])]
    stores = [pltpu.make_async_copy(vs.at[pl.ds(0, PIECE)], dw1, out_sem.at[0])]
    for k, (src, mid, dst) in enumerate(((dw3_in, v3, dw3), (dw2_in, v2, dw2))):
        for part in range(2):
            rows = pl.ds(part * TILE // 2, TILE // 2)
            i = 1 + 2 * k + part
            loads.append(pltpu.make_async_copy(src.at[rows], mid.at[rows], in_sem.at[i]))
            stores.append(pltpu.make_async_copy(mid.at[rows], dst.at[rows], out_sem.at[i]))
    for load in loads:
        load.start()
    for load, store in zip(loads, stores):
        load.wait()
        store.start()
    for k, ref in enumerate((gs2, gg2, gs1, gg1)):
        stores.append(pltpu.make_async_copy(vs.at[pl.ds(PIECE + k, 1), :], ref, out_sem.at[5 + k]))
        stores[-1].start()
    loss[...] = vs[pl.ds(PIECE + 4, 1), pl.ds(0, 1)]
    for store in stores:
        store.wait()


VMEM_SPEC = pl.BlockSpec(memory_space=pltpu.VMEM)
ANY_SPEC = pl.BlockSpec(memory_space=pl.ANY)
SMEM_SPEC = pl.BlockSpec(memory_space=pltpu.SMEM)
DMA = pltpu.SemaphoreType.DMA


def params(collective_id):
    return pltpu.CompilerParams(collective_id=collective_id, has_side_effects=True, vmem_limit_bytes=64_000_000)


def solution(mesh):
    sds = jax.ShapeDtypeStruct
    normed = sds((2, FWD_TILES, VIEW, FWD_TILE), F32)
    act = sds((ROWS, WIDTH), BF16)
    weight = sds((TILE, WIDTH), F32)
    vector = sds((1, WIDTH), F32)
    small = 2 * PIECE - 40
    small_inputs = [pltpu.VMEM((VIEW, FEAT), BF16)] * 2 + [pltpu.VMEM((1, WIDTH), F32)] * 4

    def local_step(h_a, h_b, w_one, w_two, w_three, gain_one, shift_one, gain_two, shift_two, lam_off):
        g1, b1, g2, b2 = (v.reshape(1, WIDTH) for v in (gain_one, shift_one, gain_two, shift_two))
        inv, x1, x2, zh, xh1, xh2, zn = pl.pallas_call(
            forward_kernel,
            out_shape=(sds((3, 2, FWD_TILES, 1, FWD_TILE), F32), act, act, act, normed, normed, normed),
            in_specs=[ANY_SPEC] * 9,
            out_specs=(VMEM_SPEC,) + (ANY_SPEC,) * 6,
            scratch_shapes=[
                pltpu.VMEM((ROWS, WIDTH), BF16), pltpu.VMEM((ROWS, WIDTH), BF16), pltpu.VMEM((ROWS, WIDTH), BF16),
                pltpu.VMEM((FEAT, WIDTH), BF16), pltpu.VMEM((2, WIDTH, WIDTH), BF16),
                pltpu.VMEM((2, FWD_TILES, VIEW, FWD_TILE), F32), pltpu.VMEM((6 * FWD_TILES, 8, 2, FWD_TILE), F32),
            ] + small_inputs + [
                DMA, DMA((2,)), DMA((2, FWD_TILES)), DMA((3, 2, FWD_TILES)), DMA((6 * FWD_TILES,)), DMA((6 * FWD_TILES,)),
                DMA((6,)),
            ],
            compiler_params=params(0), name="forward",
        )(h_a, h_b, w_one, w_two, w_three, g1, b1, g2, b2)
        dw3, dw2, rest = pl.pallas_call(
            main_kernel,
            out_shape=(weight, weight, sds((small, WIDTH), F32)),
            in_specs=[ANY_SPEC] * 15 + [SMEM_SPEC],
            out_specs=(ANY_SPEC, ANY_SPEC, VMEM_SPEC),
            scratch_shapes=[
                pltpu.VMEM((ROWS, WIDTH), BF16), pltpu.VMEM((TILES, ROWS, TILE), F32),
                pltpu.VMEM((TILES, ROWS, TILE), F32), pltpu.VMEM((CHUNKS, 2, 2, 2, CHUNK, TILE), BF16),
                pltpu.VMEM((TILE, WIDTH), BF16),
                pltpu.VMEM((ROWS, WIDTH), BF16), pltpu.VMEM((ROWS, WIDTH), BF16), pltpu.VMEM((ROWS, WIDTH), BF16),
                pltpu.VMEM((FEAT, ROWS), BF16), pltpu.VMEM((TILE, ROWS), BF16),
                pltpu.VMEM((2, TILE, WIDTH), BF16), pltpu.VMEM((2, TILE, CHUNK), F32),
                pltpu.VMEM((1, TILE), F32), pltpu.VMEM((ST_LOSS + 1, 8, 4, TILE), F32),
            ] + small_inputs + [
                pltpu.VMEM((3, 2, FWD_TILES, 1, FWD_TILE), F32), DMA((7,)), DMA, DMA((2, TILES)), DMA((2,)), DMA((2,)), DMA((2,)), DMA((ST_LOSS + 1,)), DMA((ST_LOSS + 1,)),
            ] + [DMA((CHUNKS,))] * 6 + RING_SCRATCH,
            compiler_params=params(1), name="main",
        )(zh, zn, x2, x1, h_a, h_b, w_three, w_two, xh2, xh1, inv, g1, b1, g2, b2, lam_off.reshape(1, 1))
        dw1, dw2, dw3, gg1, gs1, gg2, gs2, loss = pl.pallas_call(
            finish_kernel,
            out_shape=(sds((PIECE, WIDTH), F32), weight, weight, vector, vector, vector, vector, sds((1, 1), F32)),
            in_specs=[ANY_SPEC] * 3,
            out_specs=(ANY_SPEC,) * 7 + (VMEM_SPEC,),
            scratch_shapes=[
                pltpu.VMEM((TILE, WIDTH), F32), pltpu.VMEM((TILE, WIDTH), F32), pltpu.VMEM((small, WIDTH), F32),
                DMA((5,)), DMA((9,)),
            ],
            compiler_params=pltpu.CompilerParams(vmem_limit_bytes=66_000_000), name="finish",
        )(dw3, dw2, rest)
        return (loss.reshape(()), dw1, dw2, dw3, gg1.reshape(WIDTH), gs1.reshape(WIDTH),
                gg2.reshape(WIDTH), gs2.reshape(WIDTH))

    row_spec = P("data", None)
    whole_mat = P(None, None)
    whole_vec = P(None)
    return jax.shard_map(
        local_step, mesh=mesh,
        in_specs=(row_spec, row_spec, whole_mat, whole_mat, whole_mat,
                  whole_vec, whole_vec, whole_vec, whole_vec, P()),
        out_specs=(P(), row_spec, row_spec, row_spec, whole_vec, whole_vec, whole_vec, whole_vec),
        check_vma=False)
```

```python
import functools

import jax
import jax.numpy as jnp
from jax import lax
from jax.experimental import pallas as pl
from jax.experimental.pallas import tpu as pltpu
from jax.sharding import PartitionSpec as P

MESH = pl.DeviceIdType.MESH
F32, BF16 = jnp.float32, jnp.bfloat16
NORM_EPS = 1e-5
TOTAL_ROWS = 4096
VIEW = 512
ROWS = 2 * VIEW
FEAT = 384
WIDTH = 2048
TILE = 256
TILES = WIDTH // TILE
FWD_TILE = 512
FWD_TILES = WIDTH // FWD_TILE
RATIO = FWD_TILE // TILE
PIECE = FEAT // 8
CHUNK = 128
CHUNKS = WIDTH // CHUNK
PER = TILE // CHUNK
PAIRS = CHUNKS // PER
LAG_C, LAG_D, LAG_F, LAG_H, LAG_I = 1, 2, 3, 4, 5
PA_SLOTS, R0_SLOTS, R1_SLOTS, R2_SLOTS = 3 * PER, PER, 2 * PER, 2 * PER


def dot_nn(a, b):
    return jnp.dot(a, b, preferred_element_type=F32)


def dot_nt(a, b):
    return lax.dot_general(a, b, (((1,), (1,)), ((), ())), preferred_element_type=F32)


def when_in(cond, fn):
    if isinstance(cond, bool):
        if cond:
            fn()
    else:
        pl.when(cond)(fn)


def peer_of(me, r):
    out = me
    for bit in (1, 2, 4):
        if r & bit:
            out = out + bit - 2 * bit * ((me // bit) % 2)
    return out


def barrier_signal(me):
    for r in range(1, 8):
        pl.semaphore_signal(pltpu.get_barrier_semaphore(), inc=1, device_id=(peer_of(me, r),), device_id_type=MESH)


def barrier_wait():
    pl.semaphore_wait(pltpu.get_barrier_semaphore(), 7)


def cols(t, width=TILE):
    if isinstance(t, int):
        return pl.ds(t * width, width)
    return pl.ds(pl.multiple_of(t * width, width), width)


def fcols(t):
    return cols(t, FWD_TILE)


def stats_send(me, st, ssem, rsem, i):
    for r in range(1, 8):
        pltpu.make_async_remote_copy(
            src_ref=st.at[i, 0], dst_ref=st.at[i, r], send_sem=ssem.at[i], recv_sem=rsem.at[i],
            device_id=(peer_of(me, r),), device_id_type=MESH).start()


def stats_wait(st, ssem, rsem, i):
    block = st.at[i, pl.ds(1, 7)]
    pltpu.make_async_copy(block, block, rsem.at[i]).wait()
    pltpu.make_async_copy(block, block, ssem.at[i]).wait()


def stats_total(st, i):
    pairs = [st[i, 2 * k] + st[i, 2 * k + 1] for k in range(4)]
    return (pairs[0] + pairs[1]) + (pairs[2] + pairs[3])


def stats_put(st, i, values, weighted):
    for v in range(values.shape[0] // VIEW):
        part = slice(v * VIEW, (v + 1) * VIEW)
        st[i, 0, pl.ds(2 * v, 1), :] = jnp.sum(values[part], axis=0, keepdims=True)
        st[i, 0, pl.ds(2 * v + 1, 1), :] = jnp.sum(weighted[part], axis=0, keepdims=True)


def copies_in(hbm, vmem, sem):
    return [pltpu.make_async_copy(src, dst, sem.at[i]) for i, (src, dst) in enumerate(zip(hbm, vmem))]


def forward_kernel(ha_hbm, hb_hbm, w1_hbm, w2_hbm, w3_hbm, g1_hbm, b1_hbm, g2_hbm, b2_hbm,
                   inv_hbm, x1_hbm, x2_hbm, zh_hbm, xh1_hbm, xh2_hbm, zn_hbm,
                   x1, x2, zh, w1, wb, u, st, h_a, h_b, g1, b1, g2, b2, inv_out, inv_sem,
                   w1_sem, w_sem, norm_sem, act_sem, ssem, rsem, in_sem):
    me = lax.axis_index("data")
    inputs = copies_in((ha_hbm, hb_hbm, g1_hbm, b1_hbm, g2_hbm, b2_hbm), (h_a, h_b, g1, b1, g2, b2), in_sem)
    w1_copy = pltpu.make_async_copy(w1_hbm, w1, w1_sem)
    w1_copy.start()
    for copy in inputs:
        copy.start()

    def w_copy(layer):
        return pltpu.make_async_copy((w2_hbm, w3_hbm)[layer], wb.at[layer], w_sem.at[layer])

    barrier_signal(me)
    w1_copy.wait()
    for copy in inputs:
        copy.wait()
    for layer in range(2):
        w_copy(layer).start()

    acts = (x1, x2, zh)
    acts_hbm = (x1_hbm, x2_hbm, zh_hbm)
    normed_hbm = (xh1_hbm, xh2_hbm, zn_hbm)

    def rows_of(v):
        return pl.ds(v * VIEW, VIEW)

    def norm_copy(layer, v, q):
        return pltpu.make_async_copy(u.at[v, q], normed_hbm[layer].at[v, q], norm_sem.at[v, q])

    def act_copy(layer, v, q):
        return pltpu.make_async_copy(acts[layer].at[rows_of(v), fcols(q)], acts_hbm[layer].at[rows_of(v), fcols(q)],
                                     act_sem.at[layer, v, q])

    def inv_copy(layer, v):
        return pltpu.make_async_copy(inv_out.at[layer, v], inv_hbm.at[layer, v], inv_sem.at[layer, v])

    def slot(layer, v, q):
        return (2 * layer + v) * FWD_TILES + q

    def run(matmul=None, norm=None):
        def body(q, carry):
            if matmul is not None:
                layer, v = matmul
                if layer > 0:
                    norm_copy(layer - 1, v, q).wait()
            if norm is not None:
                n_layer, n_view = norm
                stats_wait(st, ssem, rsem, slot(n_layer, n_view, q))
            if matmul is not None:
                if layer > 0:
                    vals = dot_nn(acts[layer - 1][rows_of(v), :], wb[layer - 1, :, fcols(q)])
                else:
                    vals = dot_nn((h_a, h_b)[v][...], w1[:, fcols(q)])
            if norm is not None:
                total = stats_total(st, slot(n_layer, n_view, q)) * (1.0 / TOTAL_ROWS)
                mean = total[0:1]
                inv = lax.rsqrt(total[1:2] - mean * mean + NORM_EPS)
                inv_out[n_layer, n_view, q] = inv
                normed = (u[n_view, q] - mean) * inv
                u[n_view, q] = normed
                if n_layer < 2:
                    gain, shift = ((g1, b1), (g2, b2))[n_layer]
                    normed = jnp.maximum(gain[:, fcols(q)] * normed + shift[:, fcols(q)], 0.0)
                acts[n_layer][rows_of(n_view), fcols(q)] = normed.astype(BF16)
            if matmul is not None:
                u[v, q] = vals
                st[slot(layer, v, q), 0, pl.ds(0, 1), :] = jnp.sum(vals, axis=0, keepdims=True)
                st[slot(layer, v, q), 0, pl.ds(1, 1), :] = jnp.sum(vals * vals, axis=0, keepdims=True)
                if matmul != (0, 0):
                    stats_send(me, st, ssem, rsem, slot(layer, v, q))
            if norm is not None:
                act_copy(n_layer, n_view, q).start()
                norm_copy(n_layer, n_view, q).start()
            return carry

        if matmul in ((1, 0), (2, 0)):
            w_copy(matmul[0] - 1).wait()
        lax.fori_loop(0, FWD_TILES, body, 0)
        if norm is not None:
            inv_copy(*norm).start()

    run(matmul=(0, 0))
    barrier_wait()
    for q in range(FWD_TILES):
        stats_send(me, st, ssem, rsem, slot(0, 0, q))
    run(matmul=(0, 1))
    run(norm=(0, 0))
    run(matmul=(1, 0), norm=(0, 1))
    run(matmul=(1, 1), norm=(1, 0))
    run(matmul=(2, 0), norm=(1, 1))
    run(matmul=(2, 1), norm=(2, 0))
    run(norm=(2, 1))
    for v in range(2):
        for layer in range(3):
            inv_copy(layer, v).wait()
        for q in range(FWD_TILES):
            norm_copy(2, v, q).wait()
            for layer in range(3):
                act_copy(layer, v, q).wait()


class Ring:
    def __init__(self, me, items, pa, r0, r1, r2, sems, credits):
        self.items, self.pa, self.r0, self.r1, self.r2 = items, pa, r0, r1, r2
        self.s0, self.q0, self.s1, self.q1, self.s2, self.q2 = sems
        self.c0, self.c1, self.c2 = credits
        core = me % 2
        x, y = (me // 2) % 2, me // 4
        self.core = core
        self.f = x + core * (y - x)
        self.s = y + core * (x - y)
        x_side, y_side = me + 2 - 4 * x, me + 4 - 8 * y
        self.partner = me + 1 - 2 * core
        self.first = x_side + core * (y_side - x_side)
        self.second = y_side + core * (x_side - y_side)

    def copy(self, src, dst, send, recv, device):
        return pltpu.make_async_remote_copy(src_ref=src, dst_ref=dst, send_sem=send, recv_sem=recv,
                                            device_id=(device,), device_id_type=MESH)

    def copy0(self, t, rows):
        return self.copy(self.pa.at[t % PA_SLOTS, 1 - self.core, :, :, pl.ds(0, rows)],
                         self.r0.at[t % R0_SLOTS, :, :, pl.ds(0, rows)],
                         self.s0.at[t % R0_SLOTS], self.q0.at[t % R0_SLOTS], self.partner)

    def copy1(self, t, rows):
        return self.copy(self.pa.at[t % PA_SLOTS, self.core, 1 - self.f, :, pl.ds(0, rows)],
                         self.r1.at[t % R1_SLOTS, :, pl.ds(0, rows)],
                         self.s1.at[t % R1_SLOTS], self.q1.at[t % R1_SLOTS], self.first)

    def copy2(self, t, rows):
        return self.copy(self.pa.at[t % PA_SLOTS, self.core, self.f, 1 - self.s, pl.ds(0, rows)],
                         self.r2.at[t % R2_SLOTS, pl.ds(0, rows)],
                         self.s2.at[t % R2_SLOTS], self.q2.at[t % R2_SLOTS], self.second)

    def take_credit(self, sem, t, slots):
        when_in(t >= slots, lambda: pl.semaphore_wait(sem, 1))

    def give_credit(self, sem, t, slots, device):
        when_in(t + slots < self.items,
                lambda: pl.semaphore_signal(sem, inc=1, device_id=(device,), device_id_type=MESH))

    def send0(self, t, rows=CHUNK):
        self.take_credit(self.c0, t, R0_SLOTS)
        self.copy0(t, rows).start()

    def stage_b(self, t, rows=CHUNK):
        self.copy0(t, rows).wait()
        slot = t % PA_SLOTS
        for k in range(4):
            a, b = k // 2, k % 2
            self.pa[slot, self.core, a, b, :rows] += self.r0[t % R0_SLOTS, a, b, :rows]
        self.give_credit(self.c0, t, R0_SLOTS, self.partner)
        self.take_credit(self.c1, t, R1_SLOTS)
        self.copy1(t, rows).start()

    def stage_c(self, t, rows=CHUNK):
        self.copy1(t, rows).wait()
        slot = t % PA_SLOTS
        for b in range(2):
            self.pa[slot, self.core, self.f, b, :rows] += self.r1[t % R1_SLOTS, b, :rows]
        self.give_credit(self.c1, t, R1_SLOTS, self.first)
        self.take_credit(self.c2, t, R2_SLOTS)
        self.copy2(t, rows).start()

    def stage_d(self, t, rows=CHUNK):
        self.copy2(t, rows).wait()
        total = self.pa[t % PA_SLOTS, self.core, self.f, self.s, :rows] + self.r2[t % R2_SLOTS, :rows]
        self.give_credit(self.c2, t, R2_SLOTS, self.second)
        return total

    def partial(self, p, lt, right):
        for chip in range(4):
            part = dot_nn(lt, right[:, pl.ds(2 * chip * TILE, 2 * TILE)])
            x, y = chip % 2, chip // 2
            for c in range(2):
                a, b = (y, x) if c else (x, y)
                for k in range(PER):
                    self.pa[(PER * p + k) % PA_SLOTS, c, a, b] = part[k * CHUNK:(k + 1) * CHUNK, c * TILE:(c + 1) * TILE]

    def send_tick(self, p):
        for k in range(PER):
            self.send0(PER * p + k)


RING_SCRATCH = [
    pltpu.VMEM((PA_SLOTS, 2, 2, 2, CHUNK, TILE), F32),
    pltpu.VMEM((R0_SLOTS, 2, 2, CHUNK, TILE), F32),
    pltpu.VMEM((R1_SLOTS, 2, CHUNK, TILE), F32),
    pltpu.VMEM((R2_SLOTS, CHUNK, TILE), F32),
    pltpu.SemaphoreType.DMA((R0_SLOTS,)), pltpu.SemaphoreType.DMA((R0_SLOTS,)),
    pltpu.SemaphoreType.DMA((R1_SLOTS,)), pltpu.SemaphoreType.DMA((R1_SLOTS,)),
    pltpu.SemaphoreType.DMA((R2_SLOTS,)), pltpu.SemaphoreType.DMA((R2_SLOTS,)),
    pltpu.SemaphoreType.REGULAR, pltpu.SemaphoreType.REGULAR, pltpu.SemaphoreType.REGULAR,
]


LAST_COLS = 1024 // PER
LAST_ITEMS = WIDTH // LAST_COLS
LAST_ROWS = LAST_COLS // TILE * PIECE
FIRST_LAST = 3 * CHUNKS
ITEMS = FIRST_LAST + LAST_ITEMS
NORM_LAG = 2
ST_LOSS = 4 * TILES


def main_kernel(zh_hbm, zn_hbm, x2_hbm, x1_hbm, ha_hbm, hb_hbm, w3_hbm, w2_hbm, xh2_hbm, xh1_hbm,
                inv_hbm, g1_hbm, b1_hbm, g2_hbm, b2_hbm, lam, dw3_hbm, dw2_hbm, small_hbm,
                z, normed, acc, gt, gbuf, x2, x1, du2, ht, lt, wt, stage, loss_acc, st,
                h_a, h_b, g1, b1, g2, b2, inv, small, small_sem, in_sem,
                z_sem, normed_sem, x_sem, w_sem, out_sem, ssem, rsem,
                es, er, fs, fr, hs, hr, *ring_refs):
    me = lax.axis_index("data")
    z_copy = pltpu.make_async_copy(zh_hbm, z, z_sem)
    x2_copy = pltpu.make_async_copy(x2_hbm, x2, x_sem.at[0])
    x1_copy = pltpu.make_async_copy(x1_hbm, x1, x_sem.at[1])

    def normed_copies(src, sem):
        return [pltpu.make_async_copy(
            src.at[v, q // RATIO, :, cols(q % RATIO)], normed.at[q, pl.ds(v * VIEW, VIEW)], sem.at[v, q])
            for v in range(2) for q in range(TILES)]

    z_copy.start()
    barrier_signal(me)
    ring = Ring(me, ITEMS, *ring_refs[:4], ring_refs[4:10], ring_refs[10:])
    core, f, s = ring.core, ring.f, ring.s
    lam_val = lam[0, 0]
    z_copy.wait()
    for copy in normed_copies(zn_hbm, normed_sem):
        copy.start()
    inputs = copies_in((ha_hbm, hb_hbm, g1_hbm, b1_hbm, g2_hbm, b2_hbm, inv_hbm),
                       (h_a, h_b, g1, b1, g2, b2, inv), in_sem)
    for copy in inputs:
        copy.start()
    x2_copy.start()
    x1_copy.start()
    view_a, view_b = pl.ds(0, VIEW), pl.ds(VIEW, VIEW)

    def copy_e(t):
        block = gt.at[t, core, f, s]
        return ring.copy(block, block, es.at[t], er.at[t], ring.second)

    def copy_f(t):
        block = gt.at[t, core, f]
        return ring.copy(block, block, fs.at[t], fr.at[t], ring.first)

    def copy_h(t):
        block = gt.at[t, core]
        return ring.copy(block, block, hs.at[t], hr.at[t], ring.partner)

    def each(work):
        def run(p):
            for k in range(PER):
                work(PER * p + k)
        return run

    def corr_partial(p):
        lt[:, view_a] = z[view_b, cols(p)].T
        ring.partial(p, lt[:, view_a], z.at[view_a])

    def corr_send(p):
        ring.send_tick(p)
        each(ring.stage_b)(p)

    def corr_a(p):
        corr_partial(p)
        corr_send(p)

    def corr_d(t):
        corr = ring.stage_d(t) * (1.0 / TOTAL_ROWS)
        diag = (lax.broadcasted_iota(jnp.int32, corr.shape, 0) + CHUNK * t
                == lax.broadcasted_iota(jnp.int32, corr.shape, 1) + TILE * me)
        gap = 1.0 - corr
        loss_acc[...] += jnp.sum(jnp.where(diag, gap * gap, lam_val * corr * corr), axis=0, keepdims=True)
        grad = jnp.where(diag, -2.0 * gap, (2.0 * lam_val) * corr)
        gt[t, core, f, s] = (grad * (1.0 / TOTAL_ROWS)).astype(BF16)
        copy_e(t).start()

    def corr_f(t):
        copy_e(t).wait()
        copy_f(t).start()

    def corr_h(t):
        copy_f(t).wait()
        copy_h(t).start()

    def corr_i(p):
        each(lambda t: copy_h(t).wait())(p)
        for dev in range(8):
            c, x, y = dev % 2, (dev // 2) % 2, dev // 4
            a, b = (y, x) if c else (x, y)
            for k in range(PER):
                gbuf[pl.ds(k * CHUNK, CHUNK), cols(dev)] = gt[PER * p + k, c, a, b]
        grad_b = dot_nt(z[view_a, :], gbuf[...])
        acc[p, view_b, :] = grad_b
        for k in range(4):
            part = dot_nn(z[view_b, cols(p)], gbuf[:, pl.ds(2 * k * TILE, 2 * TILE)])
            acc[2 * k, view_a, :] += part[:, :TILE]
            acc[2 * k + 1, view_a, :] += part[:, TILE:]
        both_views = normed_copies(zn_hbm, normed_sem)

        @pl.when(p == 0)
        def _():
            for copy in both_views:
                copy.wait()

        stats_put(st, TILES + p, grad_b, grad_b * normed[p, view_b, :])
        stats_send(me, st, ssem, rsem, TILES + p)

    def corr_tick(p, carry):
        last = PAIRS - 1
        for lag, work, end in ((0, corr_a, last), (LAG_C, each(ring.stage_c), last), (LAG_D, each(corr_d), last),
                               (LAG_F, each(corr_f), last), (LAG_I, corr_i, last - 2),
                               (LAG_H, each(corr_h), last), (LAG_I, corr_i, last)):
            item = p - lag
            start = {0: 1, LAG_I: 0 if end < last else last - 1}.get(lag, 0)
            pl.when((item >= start) & (item <= end))(functools.partial(work, item))
        return carry

    corr_partial(0)
    barrier_wait()
    corr_send(0)
    acc[...] = jnp.zeros_like(acc)
    loss_acc[...] = jnp.zeros_like(loss_acc)
    st[:, 0] = jnp.zeros((st.shape[0],) + st.shape[2:], F32)
    lax.fori_loop(1, PAIRS + LAG_I, corr_tick, 0)

    def out_sums(q, carry):
        grad = acc[q, view_a, :]
        stats_put(st, q, grad, grad * normed[q, view_a, :])
        stats_send(me, st, ssem, rsem, q)
        return carry

    lax.fori_loop(0, TILES, out_sums, 0)

    def out_norm(q, carry):
        for v in range(2):
            stats_wait(st, ssem, rsem, v * TILES + q)
            total = stats_total(st, v * TILES + q) * (1.0 / TOTAL_ROWS)
            rows = pl.ds(v * VIEW, VIEW)
            grad = acc[q, rows, :] - (total[0:1] + normed[q, rows, :] * total[1:2])
            z[rows, cols(q)] = (inv[2, v, q // RATIO, :, cols(q % RATIO)] * grad).astype(BF16)
        return carry

    for copy in inputs:
        copy.wait()
    out_norm(0, 0)
    x2_copy.wait()

    def out_copy(t, hbm):
        return pltpu.make_async_copy(stage.at[t % 2], hbm.at[:, cols(t % CHUNKS, CHUNK)], out_sem.at[t % 2])

    def store_out(t):
        when_in(t >= CHUNKS + 2, lambda: out_copy(t - 2, dw3_hbm).wait())
        stage[t % 2] = ring.stage_d(t).T
        if isinstance(t, int):
            out_copy(t, dw2_hbm if t >= 2 * CHUNKS else dw3_hbm).start()
        else:
            pl.when(t < 2 * CHUNKS)(lambda: out_copy(t, dw3_hbm).start())
            pl.when(t >= 2 * CHUNKS)(lambda: out_copy(t, dw2_hbm).start())

    gpre = acc
    for g in range(2):
        left, right, grad_out = ((z, x2, du2), (du2, x1, z))[g]
        w_hbm, xh_hbm = ((w3_hbm, xh2_hbm), (w2_hbm, xh1_hbm))[g]
        gain_ref, shift_ref = ((g2, b2), (g1, b1))[g]
        base = (2 + g) * TILES

        def w_copy(e, w_hbm=w_hbm):
            rows = e * TILE if isinstance(e, int) else pl.multiple_of(e * TILE, TILE)
            return pltpu.make_async_copy(w_hbm.at[pl.ds(rows, TILE), :], wt.at[e % 2], w_sem.at[e % 2])

        def grad_step(e, grad, norm, g=g, left=left, w_copy=w_copy, base=base, grad_out=grad_out,
                      gain_ref=gain_ref, shift_ref=shift_ref):
            d = e - NORM_LAG
            if grad:
                w_copy(e).wait()
            if norm:
                stats_wait(st, ssem, rsem, base + d)
            if grad:
                vals = dot_nt(left[...], wt[e % 2])
            if norm:
                total = stats_total(st, base + d)
                for k in range(2):
                    small[pl.ds(PIECE + 2 * g + k, 1), cols(d)] = total[k:k + 1] + total[k + 2:k + 3]
                total = total * (1.0 / TOTAL_ROWS)
                for v in range(2):
                    rows = pl.ds(v * VIEW, VIEW)
                    out = gpre[d, rows, :] - (
                        total[2 * v:2 * v + 1] + normed[d, rows, :] * total[2 * v + 1:2 * v + 2])
                    scale = gain_ref[:, cols(d)] * inv[1 - g, v, d // RATIO, :, cols(d % RATIO)]
                    grad_out[rows, cols(d)] = (scale * out).astype(BF16)
            if grad:
                values = normed[e]
                pre = gain_ref[:, cols(e)] * values + shift_ref[:, cols(e)]
                vals = jnp.where(pre > 0, vals, 0.0)
                gpre[e] = vals
                stats_put(st, base + e, vals, vals * values)
                stats_send(me, st, ssem, rsem, base + e)
                pl.when(e + 2 < TILES)(lambda: w_copy(e + 2).start())

        def tick(q, carry, g=g, left=left, right=right, grad_step=grad_step, w_copy=w_copy,
                 xh_hbm=xh_hbm):
            p = (1 + g) * PAIRS + q
            lt[...] = left[:, cols(q)].T
            ring.partial(p, lt[...], right)
            ring.send_tick(p)
            each(ring.stage_b)(p)

            @pl.when(q == 0)
            def _():
                if g == 0:
                    lax.fori_loop(1, TILES, out_norm, 0)
                w_copy(0).start()
                w_copy(1).start()
                for copy in normed_copies(xh_hbm, normed_sem):
                    copy.start()

            @pl.when(q == 1)
            def _():
                for copy in normed_copies(xh_hbm, normed_sem):
                    copy.wait()

            def step(e, carry):
                pl.when(e < NORM_LAG)(lambda: grad_step(e, True, False))
                pl.when((e >= NORM_LAG) & (e < TILES))(lambda: grad_step(e, True, True))
                pl.when(e >= TILES)(lambda: grad_step(e, False, True))
                return carry

            @pl.when(q >= 1)
            def _():
                lax.fori_loop((q - 1) * 3 // 2, q * 3 // 2, step, 0)

            if g == 0:
                pl.when(q >= LAG_C)(lambda: each(ring.stage_c)(p - LAG_C))
                pl.when(q >= LAG_D)(lambda: each(store_out)(p - LAG_D))
            else:
                each(ring.stage_c)(p - LAG_C)
                each(store_out)(p - LAG_D)
            return carry

        if g == 1:
            x1_copy.wait()
        lax.fori_loop(0, PAIRS, tick, 0)

    ht[:, view_a] = h_a[...].T
    ht[:, view_b] = h_b[...].T
    per_item = LAST_COLS // TILE

    def rows_of(t):
        return LAST_ROWS if t >= FIRST_LAST else CHUNK

    def part_copy(k):
        block = (pl.ds(0, PIECE), pl.ds(k * LAST_COLS, LAST_COLS))
        return pltpu.make_async_copy(small.at[block], small_hbm.at[block], small_sem.at[k])

    sums_rows = (pl.ds(PIECE, 8), slice(None))
    sums_copy = pltpu.make_async_copy(small.at[sums_rows], small_hbm.at[sums_rows], small_sem.at[LAST_ITEMS])
    for t in range(FIRST_LAST, ITEMS + PER * LAG_D):
        if t < ITEMS:
            for m in range(per_item):
                part = dot_nn(ht[...], z[:, cols((t - FIRST_LAST) * per_item + m)])
                for dev in range(8):
                    c, x, y = dev % 2, (dev // 2) % 2, dev // 4
                    a, b = (y, x) if c else (x, y)
                    ring.pa[t % PA_SLOTS, c, a, b, m * PIECE:(m + 1) * PIECE] = part[dev * PIECE:(dev + 1) * PIECE]
            ring.send0(t, LAST_ROWS)
            ring.stage_b(t, LAST_ROWS)
        if t - PER * LAG_C < ITEMS:
            ring.stage_c(t - PER * LAG_C, rows_of(t - PER * LAG_C))
        d = t - PER * LAG_D
        if d < FIRST_LAST:
            store_out(d)
        else:
            total = ring.stage_d(d, LAST_ROWS)
            for m in range(per_item):
                small[pl.ds(0, PIECE), cols((d - FIRST_LAST) * per_item + m)] = total[m * PIECE:(m + 1) * PIECE]
            part_copy(d - FIRST_LAST).start()
        if t == FIRST_LAST + 4:
            stats_wait(st, ssem, rsem, ST_LOSS)
            loss = jnp.sum(stats_total(st, ST_LOSS), keepdims=True)
            small[pl.ds(PIECE + 4, 4), :] = jnp.broadcast_to(loss, (4, WIDTH))
            sums_copy.start()
        if t == FIRST_LAST:
            st[ST_LOSS, 0, pl.ds(0, 1), :] = loss_acc[...]
            stats_send(me, st, ssem, rsem, ST_LOSS)
    for t in (FIRST_LAST - 2, FIRST_LAST - 1):
        out_copy(t, dw2_hbm).wait()
    sums_copy.wait()
    for k in range(LAST_ITEMS):
        part_copy(k).wait()


def finish_kernel(dw3_in, dw2_in, small_in, dw1, dw2, dw3, gg1, gs1, gg2, gs2, loss, v3, v2, vs, in_sem, out_sem):
    loads = [pltpu.make_async_copy(small_in, vs, in_sem.at[0])]
    stores = [pltpu.make_async_copy(vs.at[pl.ds(0, PIECE)], dw1, out_sem.at[0])]
    for k, (src, mid, dst) in enumerate(((dw3_in, v3, dw3), (dw2_in, v2, dw2))):
        for part in range(2):
            rows = pl.ds(part * TILE // 2, TILE // 2)
            i = 1 + 2 * k + part
            loads.append(pltpu.make_async_copy(src.at[rows], mid.at[rows], in_sem.at[i]))
            stores.append(pltpu.make_async_copy(mid.at[rows], dst.at[rows], out_sem.at[i]))
    for load in loads:
        load.start()
    for load, store in zip(loads, stores):
        load.wait()
        store.start()
    for k, ref in enumerate((gs2, gg2, gs1, gg1)):
        stores.append(pltpu.make_async_copy(vs.at[pl.ds(PIECE + k, 1), :], ref, out_sem.at[5 + k]))
        stores[-1].start()
    loss[...] = vs[pl.ds(PIECE + 4, 1), pl.ds(0, 1)]
    for store in stores:
        store.wait()


VMEM_SPEC = pl.BlockSpec(memory_space=pltpu.VMEM)
ANY_SPEC = pl.BlockSpec(memory_space=pl.ANY)
SMEM_SPEC = pl.BlockSpec(memory_space=pltpu.SMEM)
DMA = pltpu.SemaphoreType.DMA


def params(collective_id):
    return pltpu.CompilerParams(collective_id=collective_id, has_side_effects=True, vmem_limit_bytes=64_000_000)


def solution(mesh):
    sds = jax.ShapeDtypeStruct
    normed = sds((2, FWD_TILES, VIEW, FWD_TILE), F32)
    act = sds((ROWS, WIDTH), BF16)
    weight = sds((TILE, WIDTH), F32)
    vector = sds((1, WIDTH), F32)
    small = 2 * PIECE - 40
    small_inputs = [pltpu.VMEM((VIEW, FEAT), BF16)] * 2 + [pltpu.VMEM((1, WIDTH), F32)] * 4

    def local_step(h_a, h_b, w_one, w_two, w_three, gain_one, shift_one, gain_two, shift_two, lam_off):
        g1, b1, g2, b2 = (v.reshape(1, WIDTH) for v in (gain_one, shift_one, gain_two, shift_two))
        inv, x1, x2, zh, xh1, xh2, zn = pl.pallas_call(
            forward_kernel,
            out_shape=(sds((3, 2, FWD_TILES, 1, FWD_TILE), F32), act, act, act, normed, normed, normed),
            in_specs=[ANY_SPEC] * 9,
            out_specs=(ANY_SPEC,) * 7,
            scratch_shapes=[
                pltpu.VMEM((ROWS, WIDTH), BF16), pltpu.VMEM((ROWS, WIDTH), BF16), pltpu.VMEM((ROWS, WIDTH), BF16),
                pltpu.VMEM((FEAT, WIDTH), BF16), pltpu.VMEM((2, WIDTH, WIDTH), BF16),
                pltpu.VMEM((2, FWD_TILES, VIEW, FWD_TILE), F32), pltpu.VMEM((6 * FWD_TILES, 8, 2, FWD_TILE), F32),
            ] + small_inputs + [
                pltpu.VMEM((3, 2, FWD_TILES, 1, FWD_TILE), F32), DMA((3, 2)),
                DMA, DMA((2,)), DMA((2, FWD_TILES)), DMA((3, 2, FWD_TILES)), DMA((6 * FWD_TILES,)), DMA((6 * FWD_TILES,)),
                DMA((6,)),
            ],
            compiler_params=params(0), name="forward",
        )(h_a, h_b, w_one, w_two, w_three, g1, b1, g2, b2)
        dw3, dw2, rest = pl.pallas_call(
            main_kernel,
            out_shape=(weight, weight, sds((small, WIDTH), F32)),
            in_specs=[ANY_SPEC] * 15 + [SMEM_SPEC],
            out_specs=(ANY_SPEC,) * 3,
            scratch_shapes=[
                pltpu.VMEM((ROWS, WIDTH), BF16), pltpu.VMEM((TILES, ROWS, TILE), F32),
                pltpu.VMEM((TILES, ROWS, TILE), F32), pltpu.VMEM((CHUNKS, 2, 2, 2, CHUNK, TILE), BF16),
                pltpu.VMEM((TILE, WIDTH), BF16),
                pltpu.VMEM((ROWS, WIDTH), BF16), pltpu.VMEM((ROWS, WIDTH), BF16), pltpu.VMEM((ROWS, WIDTH), BF16),
                pltpu.VMEM((FEAT, ROWS), BF16), pltpu.VMEM((TILE, ROWS), BF16),
                pltpu.VMEM((2, TILE, WIDTH), BF16), pltpu.VMEM((2, TILE, CHUNK), F32),
                pltpu.VMEM((1, TILE), F32), pltpu.VMEM((ST_LOSS + 1, 8, 4, TILE), F32),
            ] + small_inputs + [
                pltpu.VMEM((3, 2, FWD_TILES, 1, FWD_TILE), F32),
                pltpu.VMEM((small, WIDTH), F32), DMA((LAST_ITEMS + 1,)), DMA((7,)), DMA, DMA((2, TILES)), DMA((2,)), DMA((2,)), DMA((2,)), DMA((ST_LOSS + 1,)), DMA((ST_LOSS + 1,)),
            ] + [DMA((CHUNKS,))] * 6 + RING_SCRATCH,
            compiler_params=params(1), name="main",
        )(zh, zn, x2, x1, h_a, h_b, w_three, w_two, xh2, xh1, inv, g1, b1, g2, b2, lam_off.reshape(1, 1))
        dw1, dw2, dw3, gg1, gs1, gg2, gs2, loss = pl.pallas_call(
            finish_kernel,
            out_shape=(sds((PIECE, WIDTH), F32), weight, weight, vector, vector, vector, vector, sds((1, 1), F32)),
            in_specs=[ANY_SPEC] * 3,
            out_specs=(ANY_SPEC,) * 7 + (VMEM_SPEC,),
            scratch_shapes=[
                pltpu.VMEM((TILE, WIDTH), F32), pltpu.VMEM((TILE, WIDTH), F32), pltpu.VMEM((small, WIDTH), F32),
                DMA((5,)), DMA((9,)),
            ],
            compiler_params=pltpu.CompilerParams(vmem_limit_bytes=66_000_000), name="finish",
        )(dw3, dw2, rest)
        return (loss.reshape(()), dw1, dw2, dw3, gg1.reshape(WIDTH), gs1.reshape(WIDTH),
                gg2.reshape(WIDTH), gs2.reshape(WIDTH))

    row_spec = P("data", None)
    whole_mat = P(None, None)
    whole_vec = P(None)
    return jax.shard_map(
        local_step, mesh=mesh,
        in_specs=(row_spec, row_spec, whole_mat, whole_mat, whole_mat,
                  whole_vec, whole_vec, whole_vec, whole_vec, P()),
        out_specs=(P(), row_spec, row_spec, row_spec, whole_vec, whole_vec, whole_vec, whole_vec),
        check_vma=False)
```

```python
import functools

import jax
import jax.numpy as jnp
from jax import lax
from jax.experimental import pallas as pl
from jax.experimental.pallas import tpu as pltpu
from jax.sharding import PartitionSpec as P

MESH = pl.DeviceIdType.MESH
F32, BF16 = jnp.float32, jnp.bfloat16
NORM_EPS = 1e-5
TOTAL_ROWS = 4096
VIEW = 512
ROWS = 2 * VIEW
FEAT = 384
WIDTH = 2048
TILE = 256
TILES = WIDTH // TILE
FWD_TILE = 512
FWD_TILES = WIDTH // FWD_TILE
RATIO = FWD_TILE // TILE
PIECE = FEAT // 8
CHUNK = 128
CHUNKS = WIDTH // CHUNK
PER = TILE // CHUNK
PAIRS = CHUNKS // PER
LAG_C, LAG_D, LAG_F, LAG_H, LAG_I = 1, 2, 3, 4, 5
PA_SLOTS, R0_SLOTS, R1_SLOTS, R2_SLOTS = 3 * PER, PER, 2 * PER, 2 * PER


def dot_nn(a, b):
    return jnp.dot(a, b, preferred_element_type=F32)


def dot_nt(a, b):
    return lax.dot_general(a, b, (((1,), (1,)), ((), ())), preferred_element_type=F32)


def when_in(cond, fn):
    if isinstance(cond, bool):
        if cond:
            fn()
    else:
        pl.when(cond)(fn)


def peer_of(me, r):
    out = me
    for bit in (1, 2, 4):
        if r & bit:
            out = out + bit - 2 * bit * ((me // bit) % 2)
    return out


def barrier_signal(me):
    for r in range(1, 8):
        pl.semaphore_signal(pltpu.get_barrier_semaphore(), inc=1, device_id=(peer_of(me, r),), device_id_type=MESH)


def barrier_wait():
    pl.semaphore_wait(pltpu.get_barrier_semaphore(), 7)


def cols(t, width=TILE):
    if isinstance(t, int):
        return pl.ds(t * width, width)
    return pl.ds(pl.multiple_of(t * width, width), width)


def fcols(t):
    return cols(t, FWD_TILE)


def stats_send(me, st, ssem, rsem, i):
    for r in range(1, 8):
        pltpu.make_async_remote_copy(
            src_ref=st.at[i, 0], dst_ref=st.at[i, r], send_sem=ssem.at[i], recv_sem=rsem.at[i],
            device_id=(peer_of(me, r),), device_id_type=MESH).start()


def stats_wait(st, ssem, rsem, i):
    block = st.at[i, pl.ds(1, 7)]
    pltpu.make_async_copy(block, block, rsem.at[i]).wait()
    pltpu.make_async_copy(block, block, ssem.at[i]).wait()


def stats_total(st, i):
    pairs = [st[i, 2 * k] + st[i, 2 * k + 1] for k in range(4)]
    return (pairs[0] + pairs[1]) + (pairs[2] + pairs[3])


def stats_put(st, i, values, weighted):
    for v in range(values.shape[0] // VIEW):
        part = slice(v * VIEW, (v + 1) * VIEW)
        st[i, 0, pl.ds(2 * v, 1), :] = jnp.sum(values[part], axis=0, keepdims=True)
        st[i, 0, pl.ds(2 * v + 1, 1), :] = jnp.sum(weighted[part], axis=0, keepdims=True)


def copies_in(hbm, vmem, sem):
    return [pltpu.make_async_copy(src, dst, sem.at[i]) for i, (src, dst) in enumerate(zip(hbm, vmem))]


def forward_kernel(ha_hbm, hb_hbm, w1_hbm, w2_hbm, w3_hbm, g1_hbm, b1_hbm, g2_hbm, b2_hbm,
                   inv_hbm, x1_hbm, x2_hbm, zh_hbm, xh1_hbm, xh2_hbm, zn_hbm,
                   x1, x2, zh, w1, wb, u, st, h_a, h_b, g1, b1, g2, b2, inv_out, inv_sem,
                   w1_sem, w_sem, norm_sem, act_sem, ssem, rsem, in_sem):
    me = lax.axis_index("data")
    inputs = copies_in((ha_hbm, hb_hbm, g1_hbm, b1_hbm, g2_hbm, b2_hbm), (h_a, h_b, g1, b1, g2, b2), in_sem)
    w1_copy = pltpu.make_async_copy(w1_hbm, w1, w1_sem)
    w1_copy.start()
    for copy in inputs:
        copy.start()

    def w_copy(layer):
        return pltpu.make_async_copy((w2_hbm, w3_hbm)[layer], wb.at[layer], w_sem.at[layer])

    barrier_signal(me)
    w1_copy.wait()
    for copy in inputs:
        copy.wait()
    for layer in range(2):
        w_copy(layer).start()

    acts = (x1, x2, zh)
    acts_hbm = (x1_hbm, x2_hbm, zh_hbm)
    normed_hbm = (xh1_hbm, xh2_hbm, zn_hbm)

    def rows_of(v):
        return pl.ds(v * VIEW, VIEW)

    def norm_copy(layer, v, q):
        return pltpu.make_async_copy(u.at[v, q], normed_hbm[layer].at[v, q], norm_sem.at[v, q])

    def act_copy(layer, v, q):
        return pltpu.make_async_copy(acts[layer].at[rows_of(v), fcols(q)], acts_hbm[layer].at[rows_of(v), fcols(q)],
                                     act_sem.at[layer, v, q])

    def inv_copy(layer, v):
        return pltpu.make_async_copy(inv_out.at[layer, v], inv_hbm.at[layer, v], inv_sem.at[layer, v])

    def slot(layer, v, q):
        return (2 * layer + v) * FWD_TILES + q

    def run(matmul=None, norm=None):
        def body(q, carry):
            if matmul is not None:
                layer, v = matmul
                if layer > 0:
                    norm_copy(layer - 1, v, q).wait()
            if norm is not None:
                n_layer, n_view = norm
                stats_wait(st, ssem, rsem, slot(n_layer, n_view, q))
            if matmul is not None:
                if layer > 0:
                    vals = dot_nn(acts[layer - 1][rows_of(v), :], wb[layer - 1, :, fcols(q)])
                else:
                    vals = dot_nn((h_a, h_b)[v][...], w1[:, fcols(q)])
            if norm is not None:
                total = stats_total(st, slot(n_layer, n_view, q)) * (1.0 / TOTAL_ROWS)
                mean = total[0:1]
                inv = lax.rsqrt(total[1:2] - mean * mean + NORM_EPS)
                inv_out[n_layer, n_view, q] = inv
                normed = (u[n_view, q] - mean) * inv
                u[n_view, q] = normed
                if n_layer < 2:
                    gain, shift = ((g1, b1), (g2, b2))[n_layer]
                    normed = jnp.maximum(gain[:, fcols(q)] * normed + shift[:, fcols(q)], 0.0)
                acts[n_layer][rows_of(n_view), fcols(q)] = normed.astype(BF16)
            if matmul is not None:
                u[v, q] = vals
                st[slot(layer, v, q), 0, pl.ds(0, 1), :] = jnp.sum(vals, axis=0, keepdims=True)
                st[slot(layer, v, q), 0, pl.ds(1, 1), :] = jnp.sum(vals * vals, axis=0, keepdims=True)
                if matmul != (0, 0):
                    stats_send(me, st, ssem, rsem, slot(layer, v, q))
            if norm is not None:
                act_copy(n_layer, n_view, q).start()
                norm_copy(n_layer, n_view, q).start()
            return carry

        if matmul in ((1, 0), (2, 0)):
            w_copy(matmul[0] - 1).wait()
        lax.fori_loop(0, FWD_TILES, body, 0)
        if norm is not None:
            inv_copy(*norm).start()

    run(matmul=(0, 0))
    barrier_wait()
    for q in range(FWD_TILES):
        stats_send(me, st, ssem, rsem, slot(0, 0, q))
    run(matmul=(0, 1))
    run(norm=(0, 0))
    run(matmul=(1, 0), norm=(0, 1))
    run(matmul=(1, 1), norm=(1, 0))
    run(matmul=(2, 0), norm=(1, 1))
    run(matmul=(2, 1), norm=(2, 0))
    run(norm=(2, 1))
    for v in range(2):
        for layer in range(3):
            inv_copy(layer, v).wait()
        for q in range(FWD_TILES):
            norm_copy(2, v, q).wait()
            for layer in range(3):
                act_copy(layer, v, q).wait()


class Ring:
    def __init__(self, me, items, pa, r0, r1, r2, sems, credits):
        self.items, self.pa, self.r0, self.r1, self.r2 = items, pa, r0, r1, r2
        self.s0, self.q0, self.s1, self.q1, self.s2, self.q2 = sems
        self.c0, self.c1, self.c2 = credits
        core = me % 2
        x, y = (me // 2) % 2, me // 4
        self.core = core
        self.f = x + core * (y - x)
        self.s = y + core * (x - y)
        x_side, y_side = me + 2 - 4 * x, me + 4 - 8 * y
        self.partner = me + 1 - 2 * core
        self.first = x_side + core * (y_side - x_side)
        self.second = y_side + core * (x_side - y_side)

    def copy(self, src, dst, send, recv, device):
        return pltpu.make_async_remote_copy(src_ref=src, dst_ref=dst, send_sem=send, recv_sem=recv,
                                            device_id=(device,), device_id_type=MESH)

    def copy0(self, t, rows):
        return self.copy(self.pa.at[t % PA_SLOTS, 1 - self.core, :, :, pl.ds(0, rows)],
                         self.r0.at[t % R0_SLOTS, :, :, pl.ds(0, rows)],
                         self.s0.at[t % R0_SLOTS], self.q0.at[t % R0_SLOTS], self.partner)

    def copy1(self, t, rows):
        return self.copy(self.pa.at[t % PA_SLOTS, self.core, 1 - self.f, :, pl.ds(0, rows)],
                         self.r1.at[t % R1_SLOTS, :, pl.ds(0, rows)],
                         self.s1.at[t % R1_SLOTS], self.q1.at[t % R1_SLOTS], self.first)

    def copy2(self, t, rows):
        return self.copy(self.pa.at[t % PA_SLOTS, self.core, self.f, 1 - self.s, pl.ds(0, rows)],
                         self.r2.at[t % R2_SLOTS, pl.ds(0, rows)],
                         self.s2.at[t % R2_SLOTS], self.q2.at[t % R2_SLOTS], self.second)

    def take_credit(self, sem, t, slots):
        when_in(t >= slots, lambda: pl.semaphore_wait(sem, 1))

    def give_credit(self, sem, t, slots, device):
        when_in(t + slots < self.items,
                lambda: pl.semaphore_signal(sem, inc=1, device_id=(device,), device_id_type=MESH))

    def send0(self, t, rows=CHUNK):
        self.take_credit(self.c0, t, R0_SLOTS)
        self.copy0(t, rows).start()

    def stage_b(self, t, rows=CHUNK):
        self.copy0(t, rows).wait()
        slot = t % PA_SLOTS
        for k in range(4):
            a, b = k // 2, k % 2
            self.pa[slot, self.core, a, b, :rows] += self.r0[t % R0_SLOTS, a, b, :rows]
        self.give_credit(self.c0, t, R0_SLOTS, self.partner)
        self.take_credit(self.c1, t, R1_SLOTS)
        self.copy1(t, rows).start()

    def stage_c(self, t, rows=CHUNK):
        self.copy1(t, rows).wait()
        slot = t % PA_SLOTS
        for b in range(2):
            self.pa[slot, self.core, self.f, b, :rows] += self.r1[t % R1_SLOTS, b, :rows]
        self.give_credit(self.c1, t, R1_SLOTS, self.first)
        self.take_credit(self.c2, t, R2_SLOTS)
        self.copy2(t, rows).start()

    def stage_d(self, t, rows=CHUNK):
        self.copy2(t, rows).wait()
        total = self.pa[t % PA_SLOTS, self.core, self.f, self.s, :rows] + self.r2[t % R2_SLOTS, :rows]
        self.give_credit(self.c2, t, R2_SLOTS, self.second)
        return total

    def partial(self, p, lt, right):
        for chip in range(4):
            part = dot_nn(lt, right[:, pl.ds(2 * chip * TILE, 2 * TILE)])
            x, y = chip % 2, chip // 2
            for c in range(2):
                a, b = (y, x) if c else (x, y)
                for k in range(PER):
                    self.pa[(PER * p + k) % PA_SLOTS, c, a, b] = part[k * CHUNK:(k + 1) * CHUNK, c * TILE:(c + 1) * TILE]

    def send_tick(self, p):
        for k in range(PER):
            self.send0(PER * p + k)


RING_SCRATCH = [
    pltpu.VMEM((PA_SLOTS, 2, 2, 2, CHUNK, TILE), F32),
    pltpu.VMEM((R0_SLOTS, 2, 2, CHUNK, TILE), F32),
    pltpu.VMEM((R1_SLOTS, 2, CHUNK, TILE), F32),
    pltpu.VMEM((R2_SLOTS, CHUNK, TILE), F32),
    pltpu.SemaphoreType.DMA((R0_SLOTS,)), pltpu.SemaphoreType.DMA((R0_SLOTS,)),
    pltpu.SemaphoreType.DMA((R1_SLOTS,)), pltpu.SemaphoreType.DMA((R1_SLOTS,)),
    pltpu.SemaphoreType.DMA((R2_SLOTS,)), pltpu.SemaphoreType.DMA((R2_SLOTS,)),
    pltpu.SemaphoreType.REGULAR, pltpu.SemaphoreType.REGULAR, pltpu.SemaphoreType.REGULAR,
]


LAST_COLS = 1024 // PER
LAST_ITEMS = WIDTH // LAST_COLS
LAST_ROWS = LAST_COLS // TILE * PIECE
FIRST_LAST = 3 * CHUNKS
ITEMS = FIRST_LAST + LAST_ITEMS
NORM_LAG = 2
ST_LOSS = 4 * TILES


def main_kernel(zh_hbm, zn_hbm, x2_hbm, x1_hbm, ha_hbm, hb_hbm, w3_hbm, w2_hbm, xh2_hbm, xh1_hbm,
                inv_hbm, g1_hbm, b1_hbm, g2_hbm, b2_hbm, lam, dw3, dw2, small,
                z, normed, acc, gt, gbuf, x2, x1, du2, ht, lt, wt, loss_acc, st,
                h_a, h_b, g1, b1, g2, b2, inv, in_sem,
                z_sem, normed_sem, x_sem, w_sem, ssem, rsem,
                es, er, fs, fr, hs, hr, *ring_refs):
    me = lax.axis_index("data")
    z_copy = pltpu.make_async_copy(zh_hbm, z, z_sem)
    x2_copy = pltpu.make_async_copy(x2_hbm, x2, x_sem.at[0])
    x1_copy = pltpu.make_async_copy(x1_hbm, x1, x_sem.at[1])

    def normed_copies(src, sem):
        return [pltpu.make_async_copy(
            src.at[v, q // RATIO, :, cols(q % RATIO)], normed.at[q, pl.ds(v * VIEW, VIEW)], sem.at[v, q])
            for v in range(2) for q in range(TILES)]

    z_copy.start()
    barrier_signal(me)
    ring = Ring(me, ITEMS, *ring_refs[:4], ring_refs[4:10], ring_refs[10:])
    core, f, s = ring.core, ring.f, ring.s
    lam_val = lam[0, 0]
    z_copy.wait()
    for copy in normed_copies(zn_hbm, normed_sem):
        copy.start()
    inputs = copies_in((ha_hbm, hb_hbm, g1_hbm, b1_hbm, g2_hbm, b2_hbm, inv_hbm),
                       (h_a, h_b, g1, b1, g2, b2, inv), in_sem)
    for copy in inputs:
        copy.start()
    x2_copy.start()
    x1_copy.start()
    view_a, view_b = pl.ds(0, VIEW), pl.ds(VIEW, VIEW)

    def copy_e(t):
        block = gt.at[t, core, f, s]
        return ring.copy(block, block, es.at[t], er.at[t], ring.second)

    def copy_f(t):
        block = gt.at[t, core, f]
        return ring.copy(block, block, fs.at[t], fr.at[t], ring.first)

    def copy_h(t):
        block = gt.at[t, core]
        return ring.copy(block, block, hs.at[t], hr.at[t], ring.partner)

    def each(work):
        def run(p):
            for k in range(PER):
                work(PER * p + k)
        return run

    def corr_partial(p):
        lt[:, view_a] = z[view_b, cols(p)].T
        ring.partial(p, lt[:, view_a], z.at[view_a])

    def corr_send(p):
        ring.send_tick(p)
        each(ring.stage_b)(p)

    def corr_a(p):
        corr_partial(p)
        corr_send(p)

    def corr_d(t):
        corr = ring.stage_d(t) * (1.0 / TOTAL_ROWS)
        diag = (lax.broadcasted_iota(jnp.int32, corr.shape, 0) + CHUNK * t
                == lax.broadcasted_iota(jnp.int32, corr.shape, 1) + TILE * me)
        gap = 1.0 - corr
        loss_acc[...] += jnp.sum(jnp.where(diag, gap * gap, lam_val * corr * corr), axis=0, keepdims=True)
        grad = jnp.where(diag, -2.0 * gap, (2.0 * lam_val) * corr)
        gt[t, core, f, s] = (grad * (1.0 / TOTAL_ROWS)).astype(BF16)
        copy_e(t).start()

    def corr_f(t):
        copy_e(t).wait()
        copy_f(t).start()

    def corr_h(t):
        copy_f(t).wait()
        copy_h(t).start()

    def corr_i(p):
        each(lambda t: copy_h(t).wait())(p)
        for dev in range(8):
            c, x, y = dev % 2, (dev // 2) % 2, dev // 4
            a, b = (y, x) if c else (x, y)
            for k in range(PER):
                gbuf[pl.ds(k * CHUNK, CHUNK), cols(dev)] = gt[PER * p + k, c, a, b]
        grad_b = dot_nt(z[view_a, :], gbuf[...])
        acc[p, view_b, :] = grad_b
        for k in range(4):
            part = dot_nn(z[view_b, cols(p)], gbuf[:, pl.ds(2 * k * TILE, 2 * TILE)])
            acc[2 * k, view_a, :] += part[:, :TILE]
            acc[2 * k + 1, view_a, :] += part[:, TILE:]
        both_views = normed_copies(zn_hbm, normed_sem)

        @pl.when(p == 0)
        def _():
            for copy in both_views:
                copy.wait()

        stats_put(st, TILES + p, grad_b, grad_b * normed[p, view_b, :])
        stats_send(me, st, ssem, rsem, TILES + p)

    def corr_tick(p, carry):
        last = PAIRS - 1
        for lag, work, end in ((0, corr_a, last), (LAG_C, each(ring.stage_c), last), (LAG_D, each(corr_d), last),
                               (LAG_F, each(corr_f), last), (LAG_I, corr_i, last - 2),
                               (LAG_H, each(corr_h), last), (LAG_I, corr_i, last)):
            item = p - lag
            start = {0: 1, LAG_I: 0 if end < last else last - 1}.get(lag, 0)
            pl.when((item >= start) & (item <= end))(functools.partial(work, item))
        return carry

    corr_partial(0)
    barrier_wait()
    corr_send(0)
    acc[...] = jnp.zeros_like(acc)
    loss_acc[...] = jnp.zeros_like(loss_acc)
    st[:, 0] = jnp.zeros((st.shape[0],) + st.shape[2:], F32)
    lax.fori_loop(1, PAIRS + LAG_I, corr_tick, 0)

    def out_sums(q, carry):
        grad = acc[q, view_a, :]
        stats_put(st, q, grad, grad * normed[q, view_a, :])
        stats_send(me, st, ssem, rsem, q)
        return carry

    lax.fori_loop(0, TILES, out_sums, 0)

    def out_norm(q, carry):
        for v in range(2):
            stats_wait(st, ssem, rsem, v * TILES + q)
            total = stats_total(st, v * TILES + q) * (1.0 / TOTAL_ROWS)
            rows = pl.ds(v * VIEW, VIEW)
            grad = acc[q, rows, :] - (total[0:1] + normed[q, rows, :] * total[1:2])
            z[rows, cols(q)] = (inv[2, v, q // RATIO, :, cols(q % RATIO)] * grad).astype(BF16)
        return carry

    for copy in inputs:
        copy.wait()
    out_norm(0, 0)
    x2_copy.wait()

    def store_out(t):
        block = ring.stage_d(t).T

        def third():
            dw3[:, cols(t % CHUNKS, CHUNK)] = block

        def second():
            dw2[:, cols(t % CHUNKS, CHUNK)] = block

        when_in(t < 2 * CHUNKS, third)
        when_in(t >= 2 * CHUNKS, second)

    gpre = acc
    for g in range(2):
        left, right, grad_out = ((z, x2, du2), (du2, x1, z))[g]
        w_hbm, xh_hbm = ((w3_hbm, xh2_hbm), (w2_hbm, xh1_hbm))[g]
        gain_ref, shift_ref = ((g2, b2), (g1, b1))[g]
        base = (2 + g) * TILES

        def w_copy(e, w_hbm=w_hbm):
            rows = e * TILE if isinstance(e, int) else pl.multiple_of(e * TILE, TILE)
            return pltpu.make_async_copy(w_hbm.at[pl.ds(rows, TILE), :], wt.at[e % 2], w_sem.at[e % 2])

        def grad_step(e, grad, norm, g=g, left=left, w_copy=w_copy, base=base, grad_out=grad_out,
                      gain_ref=gain_ref, shift_ref=shift_ref):
            d = e - NORM_LAG
            if grad:
                w_copy(e).wait()
            if norm:
                stats_wait(st, ssem, rsem, base + d)
            if grad:
                vals = dot_nt(left[...], wt[e % 2])
            if norm:
                total = stats_total(st, base + d)
                for k in range(2):
                    small[pl.ds(PIECE + 2 * g + k, 1), cols(d)] = total[k:k + 1] + total[k + 2:k + 3]
                total = total * (1.0 / TOTAL_ROWS)
                for v in range(2):
                    rows = pl.ds(v * VIEW, VIEW)
                    out = gpre[d, rows, :] - (
                        total[2 * v:2 * v + 1] + normed[d, rows, :] * total[2 * v + 1:2 * v + 2])
                    scale = gain_ref[:, cols(d)] * inv[1 - g, v, d // RATIO, :, cols(d % RATIO)]
                    grad_out[rows, cols(d)] = (scale * out).astype(BF16)
            if grad:
                values = normed[e]
                pre = gain_ref[:, cols(e)] * values + shift_ref[:, cols(e)]
                vals = jnp.where(pre > 0, vals, 0.0)
                gpre[e] = vals
                stats_put(st, base + e, vals, vals * values)
                stats_send(me, st, ssem, rsem, base + e)
                pl.when(e + 2 < TILES)(lambda: w_copy(e + 2).start())

        def tick(q, carry, g=g, left=left, right=right, grad_step=grad_step, w_copy=w_copy,
                 xh_hbm=xh_hbm):
            p = (1 + g) * PAIRS + q
            lt[...] = left[:, cols(q)].T
            ring.partial(p, lt[...], right)
            ring.send_tick(p)
            each(ring.stage_b)(p)

            @pl.when(q == 0)
            def _():
                if g == 0:
                    lax.fori_loop(1, TILES, out_norm, 0)
                w_copy(0).start()
                w_copy(1).start()
                for copy in normed_copies(xh_hbm, normed_sem):
                    copy.start()

            @pl.when(q == 1)
            def _():
                for copy in normed_copies(xh_hbm, normed_sem):
                    copy.wait()

            def step(e, carry):
                pl.when(e < NORM_LAG)(lambda: grad_step(e, True, False))
                pl.when((e >= NORM_LAG) & (e < TILES))(lambda: grad_step(e, True, True))
                pl.when(e >= TILES)(lambda: grad_step(e, False, True))
                return carry

            @pl.when(q >= 1)
            def _():
                lax.fori_loop((q - 1) * 3 // 2, q * 3 // 2, step, 0)

            if g == 0:
                pl.when(q >= LAG_C)(lambda: each(ring.stage_c)(p - LAG_C))
                pl.when(q >= LAG_D)(lambda: each(store_out)(p - LAG_D))
            else:
                each(ring.stage_c)(p - LAG_C)
                each(store_out)(p - LAG_D)
            return carry

        if g == 1:
            x1_copy.wait()
        lax.fori_loop(0, PAIRS, tick, 0)

    ht[:, view_a] = h_a[...].T
    ht[:, view_b] = h_b[...].T
    per_item = LAST_COLS // TILE

    def rows_of(t):
        return LAST_ROWS if t >= FIRST_LAST else CHUNK

    for t in range(FIRST_LAST, ITEMS + PER * LAG_D):
        if t < ITEMS:
            for m in range(per_item):
                part = dot_nn(ht[...], z[:, cols((t - FIRST_LAST) * per_item + m)])
                for dev in range(8):
                    c, x, y = dev % 2, (dev // 2) % 2, dev // 4
                    a, b = (y, x) if c else (x, y)
                    ring.pa[t % PA_SLOTS, c, a, b, m * PIECE:(m + 1) * PIECE] = part[dev * PIECE:(dev + 1) * PIECE]
            ring.send0(t, LAST_ROWS)
            ring.stage_b(t, LAST_ROWS)
        if t - PER * LAG_C < ITEMS:
            ring.stage_c(t - PER * LAG_C, rows_of(t - PER * LAG_C))
        d = t - PER * LAG_D
        if d < FIRST_LAST:
            store_out(d)
        else:
            total = ring.stage_d(d, LAST_ROWS)
            for m in range(per_item):
                small[pl.ds(0, PIECE), cols((d - FIRST_LAST) * per_item + m)] = total[m * PIECE:(m + 1) * PIECE]
        if t == FIRST_LAST + 4:
            stats_wait(st, ssem, rsem, ST_LOSS)
            loss = jnp.sum(stats_total(st, ST_LOSS), keepdims=True)
            small[pl.ds(PIECE + 4, 4), :] = jnp.broadcast_to(loss, (4, WIDTH))
        if t == FIRST_LAST:
            st[ST_LOSS, 0, pl.ds(0, 1), :] = loss_acc[...]
            stats_send(me, st, ssem, rsem, ST_LOSS)


def finish_kernel(dw3_in, dw2_in, small, dw1, dw2, dw3, gg1, gs1, gg2, gs2, loss, out_sem):
    stores = [(dw3_in, dw3), (dw2_in, dw2), (small.at[pl.ds(0, PIECE)], dw1)]
    for k, ref in enumerate((gs2, gg2, gs1, gg1)):
        stores.append((small.at[pl.ds(PIECE + k, 1), :], ref))
    stores = [pltpu.make_async_copy(src, dst, out_sem.at[k]) for k, (src, dst) in enumerate(stores)]
    for store in stores:
        store.start()
    loss[...] = small[pl.ds(PIECE + 4, 1), pl.ds(0, 1)]
    for store in stores:
        store.wait()


VMEM_SPEC = pl.BlockSpec(memory_space=pltpu.VMEM)
ANY_SPEC = pl.BlockSpec(memory_space=pl.ANY)
SMEM_SPEC = pl.BlockSpec(memory_space=pltpu.SMEM)
DMA = pltpu.SemaphoreType.DMA


def params(collective_id, limit):
    return pltpu.CompilerParams(collective_id=collective_id, has_side_effects=True, vmem_limit_bytes=limit)


def solution(mesh):
    sds = jax.ShapeDtypeStruct
    normed = sds((2, FWD_TILES, VIEW, FWD_TILE), F32)
    act = sds((ROWS, WIDTH), BF16)
    weight = sds((TILE, WIDTH), F32)
    vector = sds((1, WIDTH), F32)
    small = 2 * PIECE - 40
    small_inputs = [pltpu.VMEM((VIEW, FEAT), BF16)] * 2 + [pltpu.VMEM((1, WIDTH), F32)] * 4

    def local_step(h_a, h_b, w_one, w_two, w_three, gain_one, shift_one, gain_two, shift_two, lam_off):
        g1, b1, g2, b2 = (v.reshape(1, WIDTH) for v in (gain_one, shift_one, gain_two, shift_two))
        inv, x1, x2, zh, xh1, xh2, zn = pl.pallas_call(
            forward_kernel,
            out_shape=(sds((3, 2, FWD_TILES, 1, FWD_TILE), F32), act, act, act, normed, normed, normed),
            in_specs=[ANY_SPEC] * 9,
            out_specs=(ANY_SPEC,) * 7,
            scratch_shapes=[
                pltpu.VMEM((ROWS, WIDTH), BF16), pltpu.VMEM((ROWS, WIDTH), BF16), pltpu.VMEM((ROWS, WIDTH), BF16),
                pltpu.VMEM((FEAT, WIDTH), BF16), pltpu.VMEM((2, WIDTH, WIDTH), BF16),
                pltpu.VMEM((2, FWD_TILES, VIEW, FWD_TILE), F32), pltpu.VMEM((6 * FWD_TILES, 8, 2, FWD_TILE), F32),
            ] + small_inputs + [
                pltpu.VMEM((3, 2, FWD_TILES, 1, FWD_TILE), F32), DMA((3, 2)),
                DMA, DMA((2,)), DMA((2, FWD_TILES)), DMA((3, 2, FWD_TILES)), DMA((6 * FWD_TILES,)), DMA((6 * FWD_TILES,)),
                DMA((6,)),
            ],
            compiler_params=params(0, 64_000_000), name="forward",
        )(h_a, h_b, w_one, w_two, w_three, g1, b1, g2, b2)
        dw3, dw2, rest = pl.pallas_call(
            main_kernel,
            out_shape=(pltpu.VMEM((TILE, WIDTH), F32), pltpu.VMEM((TILE, WIDTH), F32), pltpu.VMEM((small, WIDTH), F32)),
            in_specs=[ANY_SPEC] * 15 + [SMEM_SPEC],
            out_specs=(VMEM_SPEC,) * 3,
            scratch_shapes=[
                pltpu.VMEM((ROWS, WIDTH), BF16), pltpu.VMEM((TILES, ROWS, TILE), F32),
                pltpu.VMEM((TILES, ROWS, TILE), F32), pltpu.VMEM((CHUNKS, 2, 2, 2, CHUNK, TILE), BF16),
                pltpu.VMEM((TILE, WIDTH), BF16),
                pltpu.VMEM((ROWS, WIDTH), BF16), pltpu.VMEM((ROWS, WIDTH), BF16), pltpu.VMEM((ROWS, WIDTH), BF16),
                pltpu.VMEM((FEAT, ROWS), BF16), pltpu.VMEM((TILE, ROWS), BF16),
                pltpu.VMEM((2, TILE, WIDTH), BF16),
                pltpu.VMEM((1, TILE), F32), pltpu.VMEM((ST_LOSS + 1, 8, 4, TILE), F32),
            ] + small_inputs + [
                pltpu.VMEM((3, 2, FWD_TILES, 1, FWD_TILE), F32),
                DMA((7,)), DMA, DMA((2, TILES)), DMA((2,)), DMA((2,)), DMA((ST_LOSS + 1,)), DMA((ST_LOSS + 1,)),
            ] + [DMA((CHUNKS,))] * 6 + RING_SCRATCH,
            compiler_params=params(1, 61_100_000), name="main",
        )(zh, zn, x2, x1, h_a, h_b, w_three, w_two, xh2, xh1, inv, g1, b1, g2, b2, lam_off.reshape(1, 1))
        dw1, dw2, dw3, gg1, gs1, gg2, gs2, loss = pl.pallas_call(
            finish_kernel,
            out_shape=(sds((PIECE, WIDTH), F32), weight, weight, vector, vector, vector, vector, sds((1, 1), F32)),
            in_specs=[VMEM_SPEC] * 3,
            out_specs=(ANY_SPEC,) * 7 + (VMEM_SPEC,),
            scratch_shapes=[DMA((7,))],
            compiler_params=pltpu.CompilerParams(vmem_limit_bytes=16_000_000), name="finish",
        )(dw3, dw2, rest)
        return (loss.reshape(()), dw1, dw2, dw3, gg1.reshape(WIDTH), gs1.reshape(WIDTH),
                gg2.reshape(WIDTH), gs2.reshape(WIDTH))

    row_spec = P("data", None)
    whole_mat = P(None, None)
    whole_vec = P(None)
    return jax.shard_map(
        local_step, mesh=mesh,
        in_specs=(row_spec, row_spec, whole_mat, whole_mat, whole_mat,
                  whole_vec, whole_vec, whole_vec, whole_vec, P()),
        out_specs=(P(), row_spec, row_spec, row_spec, whole_vec, whole_vec, whole_vec, whole_vec),
        check_vma=False)
```

```python
import functools

import jax
import jax.numpy as jnp
from jax import lax
from jax.experimental import pallas as pl
from jax.experimental.pallas import tpu as pltpu
from jax.sharding import PartitionSpec as P

MESH = pl.DeviceIdType.MESH
F32, BF16 = jnp.float32, jnp.bfloat16
NORM_EPS = 1e-5
TOTAL_ROWS = 4096
VIEW = 512
ROWS = 2 * VIEW
FEAT = 384
WIDTH = 2048
TILE = 256
TILES = WIDTH // TILE
FWD_TILE = 512
FWD_TILES = WIDTH // FWD_TILE
RATIO = FWD_TILE // TILE
PIECE = FEAT // 8
CHUNK = 128
CHUNKS = WIDTH // CHUNK
PER = TILE // CHUNK
PAIRS = CHUNKS // PER
LAG_C, LAG_D, LAG_F, LAG_H, LAG_I = 1, 2, 3, 4, 5
PA_SLOTS, R0_SLOTS, R1_SLOTS, R2_SLOTS = 3 * PER, PER, 2 * PER, 2 * PER


def dot_nn(a, b):
    return jnp.dot(a, b, preferred_element_type=F32)


def dot_nt(a, b):
    return lax.dot_general(a, b, (((1,), (1,)), ((), ())), preferred_element_type=F32)


def when_in(cond, fn):
    if isinstance(cond, bool):
        if cond:
            fn()
    else:
        pl.when(cond)(fn)


def peer_of(me, r):
    out = me
    for bit in (1, 2, 4):
        if r & bit:
            out = out + bit - 2 * bit * ((me // bit) % 2)
    return out


def barrier_signal(me):
    for r in range(1, 8):
        pl.semaphore_signal(pltpu.get_barrier_semaphore(), inc=1, device_id=(peer_of(me, r),), device_id_type=MESH)


def barrier_wait():
    pl.semaphore_wait(pltpu.get_barrier_semaphore(), 7)


def cols(t, width=TILE):
    if isinstance(t, int):
        return pl.ds(t * width, width)
    return pl.ds(pl.multiple_of(t * width, width), width)


def fcols(t):
    return cols(t, FWD_TILE)


def stats_send(me, st, ssem, rsem, i):
    for r in range(1, 8):
        pltpu.make_async_remote_copy(
            src_ref=st.at[i, 0], dst_ref=st.at[i, r], send_sem=ssem.at[i], recv_sem=rsem.at[i],
            device_id=(peer_of(me, r),), device_id_type=MESH).start()


def stats_wait(st, ssem, rsem, i):
    block = st.at[i, pl.ds(1, 7)]
    pltpu.make_async_copy(block, block, rsem.at[i]).wait()
    pltpu.make_async_copy(block, block, ssem.at[i]).wait()


def stats_total(st, i):
    pairs = [st[i, 2 * k] + st[i, 2 * k + 1] for k in range(4)]
    return (pairs[0] + pairs[1]) + (pairs[2] + pairs[3])


def stats_put(st, i, values, weighted):
    for v in range(values.shape[0] // VIEW):
        part = slice(v * VIEW, (v + 1) * VIEW)
        st[i, 0, pl.ds(2 * v, 1), :] = jnp.sum(values[part], axis=0, keepdims=True)
        st[i, 0, pl.ds(2 * v + 1, 1), :] = jnp.sum(weighted[part], axis=0, keepdims=True)


def copies_in(hbm, vmem, sem):
    return [pltpu.make_async_copy(src, dst, sem.at[i]) for i, (src, dst) in enumerate(zip(hbm, vmem))]


def forward_kernel(ha_hbm, hb_hbm, w1_hbm, w2_hbm, w3_hbm, g1_hbm, b1_hbm, g2_hbm, b2_hbm,
                   inv_hbm, x1_hbm, x2_hbm, zh_hbm, xh1_hbm, xh2_hbm, zn_hbm,
                   x1, x2, zh, w1, wb, u, st, h_a, h_b, g1, b1, g2, b2, inv_out, inv_sem,
                   w1_sem, w_sem, norm_sem, act_sem, ssem, rsem, in_sem):
    me = lax.axis_index("data")
    inputs = copies_in((ha_hbm, hb_hbm, g1_hbm, b1_hbm, g2_hbm, b2_hbm), (h_a, h_b, g1, b1, g2, b2), in_sem)
    w1_copy = pltpu.make_async_copy(w1_hbm, w1, w1_sem)
    w1_copy.start()
    for copy in inputs:
        copy.start()

    def w_copy(layer):
        return pltpu.make_async_copy((w2_hbm, w3_hbm)[layer], wb.at[layer], w_sem.at[layer])

    barrier_signal(me)
    w1_copy.wait()
    for copy in inputs:
        copy.wait()
    for layer in range(2):
        w_copy(layer).start()

    acts = (x1, x2, zh)
    acts_hbm = (x1_hbm, x2_hbm, zh_hbm)
    normed_hbm = (xh1_hbm, xh2_hbm, zn_hbm)

    def rows_of(v):
        return pl.ds(v * VIEW, VIEW)

    def norm_copy(layer, v, q):
        return pltpu.make_async_copy(u.at[v, q], normed_hbm[layer].at[v, q], norm_sem.at[v, q])

    def act_copy(layer, v, q):
        return pltpu.make_async_copy(acts[layer].at[rows_of(v), fcols(q)], acts_hbm[layer].at[rows_of(v), fcols(q)],
                                     act_sem.at[layer, v, q])

    def inv_copy(layer, v):
        return pltpu.make_async_copy(inv_out.at[layer, v], inv_hbm.at[layer, v], inv_sem.at[layer, v])

    def slot(layer, v, q):
        return (2 * layer + v) * FWD_TILES + q

    def run(matmul=None, norm=None):
        def body(q, carry):
            if matmul is not None:
                layer, v = matmul
                if layer > 0:
                    norm_copy(layer - 1, v, q).wait()
            if norm is not None:
                n_layer, n_view = norm
                stats_wait(st, ssem, rsem, slot(n_layer, n_view, q))
            if matmul is not None:
                if layer > 0:
                    vals = dot_nn(acts[layer - 1][rows_of(v), :], wb[layer - 1, :, fcols(q)])
                else:
                    vals = dot_nn((h_a, h_b)[v][...], w1[:, fcols(q)])
            if norm is not None:
                total = stats_total(st, slot(n_layer, n_view, q)) * (1.0 / TOTAL_ROWS)
                mean = total[0:1]
                inv = lax.rsqrt(total[1:2] - mean * mean + NORM_EPS)
                inv_out[n_layer, n_view, q] = inv
                normed = (u[n_view, q] - mean) * inv
                u[n_view, q] = normed
                if n_layer < 2:
                    gain, shift = ((g1, b1), (g2, b2))[n_layer]
                    normed = jnp.maximum(gain[:, fcols(q)] * normed + shift[:, fcols(q)], 0.0)
                acts[n_layer][rows_of(n_view), fcols(q)] = normed.astype(BF16)
            if matmul is not None:
                u[v, q] = vals
                st[slot(layer, v, q), 0, pl.ds(0, 1), :] = jnp.sum(vals, axis=0, keepdims=True)
                st[slot(layer, v, q), 0, pl.ds(1, 1), :] = jnp.sum(vals * vals, axis=0, keepdims=True)
                if matmul != (0, 0):
                    stats_send(me, st, ssem, rsem, slot(layer, v, q))
            if norm is not None:
                act_copy(n_layer, n_view, q).start()
                norm_copy(n_layer, n_view, q).start()
            return carry

        if matmul in ((1, 0), (2, 0)):
            w_copy(matmul[0] - 1).wait()
        lax.fori_loop(0, FWD_TILES, body, 0)
        if norm is not None:
            inv_copy(*norm).start()

    run(matmul=(0, 0))
    barrier_wait()
    for q in range(FWD_TILES):
        stats_send(me, st, ssem, rsem, slot(0, 0, q))
    run(matmul=(0, 1))
    run(norm=(0, 0))
    run(matmul=(1, 0), norm=(0, 1))
    run(matmul=(1, 1), norm=(1, 0))
    run(matmul=(2, 0), norm=(1, 1))
    run(matmul=(2, 1), norm=(2, 0))
    run(norm=(2, 1))
    for v in range(2):
        for layer in range(3):
            inv_copy(layer, v).wait()
        for q in range(FWD_TILES):
            norm_copy(2, v, q).wait()
            for layer in range(3):
                act_copy(layer, v, q).wait()


class Ring:
    def __init__(self, me, items, pa, r0, r1, r2, sems, credits):
        self.items, self.pa, self.r0, self.r1, self.r2 = items, pa, r0, r1, r2
        self.s0, self.q0, self.s1, self.q1, self.s2, self.q2 = sems
        self.c0, self.c1, self.c2 = credits
        core = me % 2
        x, y = (me // 2) % 2, me // 4
        self.core = core
        self.f = x + core * (y - x)
        self.s = y + core * (x - y)
        x_side, y_side = me + 2 - 4 * x, me + 4 - 8 * y
        self.partner = me + 1 - 2 * core
        self.first = x_side + core * (y_side - x_side)
        self.second = y_side + core * (x_side - y_side)

    def copy(self, src, dst, send, recv, device):
        return pltpu.make_async_remote_copy(src_ref=src, dst_ref=dst, send_sem=send, recv_sem=recv,
                                            device_id=(device,), device_id_type=MESH)

    def copy0(self, t, rows):
        return self.copy(self.pa.at[t % PA_SLOTS, 1 - self.core, :, :, pl.ds(0, rows)],
                         self.r0.at[t % R0_SLOTS, :, :, pl.ds(0, rows)],
                         self.s0.at[t % R0_SLOTS], self.q0.at[t % R0_SLOTS], self.partner)

    def copy1(self, t, rows):
        return self.copy(self.pa.at[t % PA_SLOTS, self.core, 1 - self.f, :, pl.ds(0, rows)],
                         self.r1.at[t % R1_SLOTS, :, pl.ds(0, rows)],
                         self.s1.at[t % R1_SLOTS], self.q1.at[t % R1_SLOTS], self.first)

    def copy2(self, t, rows):
        return self.copy(self.pa.at[t % PA_SLOTS, self.core, self.f, 1 - self.s, pl.ds(0, rows)],
                         self.r2.at[t % R2_SLOTS, pl.ds(0, rows)],
                         self.s2.at[t % R2_SLOTS], self.q2.at[t % R2_SLOTS], self.second)

    def take_credit(self, sem, t, slots):
        when_in(t >= slots, lambda: pl.semaphore_wait(sem, 1))

    def give_credit(self, sem, t, slots, device):
        when_in(t + slots < self.items,
                lambda: pl.semaphore_signal(sem, inc=1, device_id=(device,), device_id_type=MESH))

    def send0(self, t, rows=CHUNK):
        self.take_credit(self.c0, t, R0_SLOTS)
        self.copy0(t, rows).start()

    def stage_b(self, t, rows=CHUNK):
        self.copy0(t, rows).wait()
        slot = t % PA_SLOTS
        for k in range(4):
            a, b = k // 2, k % 2
            self.pa[slot, self.core, a, b, :rows] += self.r0[t % R0_SLOTS, a, b, :rows]
        self.give_credit(self.c0, t, R0_SLOTS, self.partner)
        self.take_credit(self.c1, t, R1_SLOTS)
        self.copy1(t, rows).start()

    def stage_c(self, t, rows=CHUNK):
        self.copy1(t, rows).wait()
        slot = t % PA_SLOTS
        for b in range(2):
            self.pa[slot, self.core, self.f, b, :rows] += self.r1[t % R1_SLOTS, b, :rows]
        self.give_credit(self.c1, t, R1_SLOTS, self.first)
        self.take_credit(self.c2, t, R2_SLOTS)
        self.copy2(t, rows).start()

    def stage_d(self, t, rows=CHUNK):
        self.copy2(t, rows).wait()
        total = self.pa[t % PA_SLOTS, self.core, self.f, self.s, :rows] + self.r2[t % R2_SLOTS, :rows]
        self.give_credit(self.c2, t, R2_SLOTS, self.second)
        return total

    def partial(self, p, lt, right):
        for chip in range(4):
            part = dot_nn(lt, right[:, pl.ds(2 * chip * TILE, 2 * TILE)])
            x, y = chip % 2, chip // 2
            for c in range(2):
                a, b = (y, x) if c else (x, y)
                for k in range(PER):
                    self.pa[(PER * p + k) % PA_SLOTS, c, a, b] = part[k * CHUNK:(k + 1) * CHUNK, c * TILE:(c + 1) * TILE]

    def send_tick(self, p):
        for k in range(PER):
            self.send0(PER * p + k)


RING_SCRATCH = [
    pltpu.VMEM((PA_SLOTS, 2, 2, 2, CHUNK, TILE), F32),
    pltpu.VMEM((R0_SLOTS, 2, 2, CHUNK, TILE), F32),
    pltpu.VMEM((R1_SLOTS, 2, CHUNK, TILE), F32),
    pltpu.VMEM((R2_SLOTS, CHUNK, TILE), F32),
    pltpu.SemaphoreType.DMA((R0_SLOTS,)), pltpu.SemaphoreType.DMA((R0_SLOTS,)),
    pltpu.SemaphoreType.DMA((R1_SLOTS,)), pltpu.SemaphoreType.DMA((R1_SLOTS,)),
    pltpu.SemaphoreType.DMA((R2_SLOTS,)), pltpu.SemaphoreType.DMA((R2_SLOTS,)),
    pltpu.SemaphoreType.REGULAR, pltpu.SemaphoreType.REGULAR, pltpu.SemaphoreType.REGULAR,
]


LAST_COLS = 1024 // PER
LAST_ITEMS = WIDTH // LAST_COLS
LAST_ROWS = LAST_COLS // TILE * PIECE
FIRST_LAST = 3 * CHUNKS
ITEMS = FIRST_LAST + LAST_ITEMS
NORM_LAG = 2
ST_LOSS = 4 * TILES


def main_kernel(zh_hbm, zn_hbm, x2_hbm, x1_hbm, ha_hbm, hb_hbm, w3_hbm, w2_hbm, xh2_hbm, xh1_hbm,
                inv_hbm, g1_hbm, b1_hbm, g2_hbm, b2_hbm, lam, dw3, dw2, small,
                z, normed, acc, gt, gbuf, x2, x1, du2, ht, lt, wt, loss_acc, st,
                h_a, h_b, g1, b1, g2, b2, inv, in_sem,
                z_sem, normed_sem, x_sem, w_sem, ssem, rsem,
                es, er, fs, fr, hs, hr, *ring_refs):
    me = lax.axis_index("data")
    blocks = ((pl.ds(0, VIEW), slice(None)), (pl.ds(VIEW, VIEW), pl.ds(0, TILE)),
              (pl.ds(VIEW, VIEW), pl.ds(TILE, WIDTH - TILE)))
    z_copies = [pltpu.make_async_copy(zh_hbm.at[b], z.at[b], z_sem.at[i]) for i, b in enumerate(blocks)]
    x2_copy = pltpu.make_async_copy(x2_hbm, x2, x_sem.at[0])
    x1_copy = pltpu.make_async_copy(x1_hbm, x1, x_sem.at[1])

    def normed_copies(src, sem):
        return [pltpu.make_async_copy(
            src.at[v, q // RATIO, :, cols(q % RATIO)], normed.at[q, pl.ds(v * VIEW, VIEW)], sem.at[v, q])
            for v in range(2) for q in range(TILES)]

    for copy in z_copies:
        copy.start()
    barrier_signal(me)
    ring = Ring(me, ITEMS, *ring_refs[:4], ring_refs[4:10], ring_refs[10:])
    core, f, s = ring.core, ring.f, ring.s
    lam_val = lam[0, 0]
    z_copies[0].wait()
    z_copies[1].wait()
    for copy in normed_copies(zn_hbm, normed_sem):
        copy.start()
    inputs = copies_in((ha_hbm, hb_hbm, g1_hbm, b1_hbm, g2_hbm, b2_hbm, inv_hbm),
                       (h_a, h_b, g1, b1, g2, b2, inv), in_sem)
    for copy in inputs:
        copy.start()
    x2_copy.start()
    x1_copy.start()
    view_a, view_b = pl.ds(0, VIEW), pl.ds(VIEW, VIEW)

    def copy_e(t):
        block = gt.at[t, core, f, s]
        return ring.copy(block, block, es.at[t], er.at[t], ring.second)

    def copy_f(t):
        block = gt.at[t, core, f]
        return ring.copy(block, block, fs.at[t], fr.at[t], ring.first)

    def copy_h(t):
        block = gt.at[t, core]
        return ring.copy(block, block, hs.at[t], hr.at[t], ring.partner)

    def each(work):
        def run(p):
            for k in range(PER):
                work(PER * p + k)
        return run

    def corr_partial(p):
        lt[:, view_a] = z[view_b, cols(p)].T
        ring.partial(p, lt[:, view_a], z.at[view_a])

    def corr_send(p):
        ring.send_tick(p)
        each(ring.stage_b)(p)

    def corr_a(p):
        corr_partial(p)
        corr_send(p)

    def corr_d(t):
        corr = ring.stage_d(t) * (1.0 / TOTAL_ROWS)
        diag = (lax.broadcasted_iota(jnp.int32, corr.shape, 0) + CHUNK * t
                == lax.broadcasted_iota(jnp.int32, corr.shape, 1) + TILE * me)
        gap = 1.0 - corr
        loss_acc[...] += jnp.sum(jnp.where(diag, gap * gap, lam_val * corr * corr), axis=0, keepdims=True)
        grad = jnp.where(diag, -2.0 * gap, (2.0 * lam_val) * corr)
        gt[t, core, f, s] = (grad * (1.0 / TOTAL_ROWS)).astype(BF16)
        copy_e(t).start()

    def corr_f(t):
        copy_e(t).wait()
        copy_f(t).start()

    def corr_h(t):
        copy_f(t).wait()
        copy_h(t).start()

    def corr_i(p):
        each(lambda t: copy_h(t).wait())(p)
        for dev in range(8):
            c, x, y = dev % 2, (dev // 2) % 2, dev // 4
            a, b = (y, x) if c else (x, y)
            for k in range(PER):
                gbuf[pl.ds(k * CHUNK, CHUNK), cols(dev)] = gt[PER * p + k, c, a, b]
        grad_b = dot_nt(z[view_a, :], gbuf[...])
        acc[p, view_b, :] = grad_b
        for k in range(4):
            part = dot_nn(z[view_b, cols(p)], gbuf[:, pl.ds(2 * k * TILE, 2 * TILE)])
            acc[2 * k, view_a, :] += part[:, :TILE]
            acc[2 * k + 1, view_a, :] += part[:, TILE:]
        both_views = normed_copies(zn_hbm, normed_sem)

        @pl.when(p == 0)
        def _():
            for copy in both_views:
                copy.wait()

        stats_put(st, TILES + p, grad_b, grad_b * normed[p, view_b, :])
        stats_send(me, st, ssem, rsem, TILES + p)

    def corr_tick(p, carry):
        last = PAIRS - 1
        for lag, work, end in ((0, corr_a, last), (LAG_C, each(ring.stage_c), last), (LAG_D, each(corr_d), last),
                               (LAG_F, each(corr_f), last), (LAG_I, corr_i, last - 2),
                               (LAG_H, each(corr_h), last), (LAG_I, corr_i, last)):
            item = p - lag
            start = {0: 1, LAG_I: 0 if end < last else last - 1}.get(lag, 0)
            pl.when((item >= start) & (item <= end))(functools.partial(work, item))
        return carry

    corr_partial(0)
    barrier_wait()
    corr_send(0)
    z_copies[2].wait()
    acc[...] = jnp.zeros_like(acc)
    loss_acc[...] = jnp.zeros_like(loss_acc)
    st[:, 0] = jnp.zeros((st.shape[0],) + st.shape[2:], F32)
    lax.fori_loop(1, PAIRS + LAG_I, corr_tick, 0)

    def out_sums(q, carry):
        grad = acc[q, view_a, :]
        stats_put(st, q, grad, grad * normed[q, view_a, :])
        stats_send(me, st, ssem, rsem, q)
        return carry

    lax.fori_loop(0, TILES, out_sums, 0)

    def out_norm(q, carry):
        for v in range(2):
            stats_wait(st, ssem, rsem, v * TILES + q)
            total = stats_total(st, v * TILES + q) * (1.0 / TOTAL_ROWS)
            rows = pl.ds(v * VIEW, VIEW)
            grad = acc[q, rows, :] - (total[0:1] + normed[q, rows, :] * total[1:2])
            z[rows, cols(q)] = (inv[2, v, q // RATIO, :, cols(q % RATIO)] * grad).astype(BF16)
        return carry

    for copy in inputs:
        copy.wait()
    out_norm(0, 0)
    x2_copy.wait()

    def store_out(t):
        block = ring.stage_d(t).T

        def third():
            dw3[:, cols(t % CHUNKS, CHUNK)] = block

        def second():
            dw2[:, cols(t % CHUNKS, CHUNK)] = block

        when_in(t < 2 * CHUNKS, third)
        when_in(t >= 2 * CHUNKS, second)

    gpre = acc
    for g in range(2):
        left, right, grad_out = ((z, x2, du2), (du2, x1, z))[g]
        w_hbm, xh_hbm = ((w3_hbm, xh2_hbm), (w2_hbm, xh1_hbm))[g]
        gain_ref, shift_ref = ((g2, b2), (g1, b1))[g]
        base = (2 + g) * TILES

        def w_copy(e, w_hbm=w_hbm):
            rows = e * TILE if isinstance(e, int) else pl.multiple_of(e * TILE, TILE)
            return pltpu.make_async_copy(w_hbm.at[pl.ds(rows, TILE), :], wt.at[e % 2], w_sem.at[e % 2])

        def grad_step(e, grad, norm, g=g, left=left, w_copy=w_copy, base=base, grad_out=grad_out,
                      gain_ref=gain_ref, shift_ref=shift_ref):
            d = e - NORM_LAG
            if grad:
                w_copy(e).wait()
            if norm:
                stats_wait(st, ssem, rsem, base + d)
            if grad:
                vals = dot_nt(left[...], wt[e % 2])
            if norm:
                total = stats_total(st, base + d)
                for k in range(2):
                    small[pl.ds(PIECE + 2 * g + k, 1), cols(d)] = total[k:k + 1] + total[k + 2:k + 3]
                total = total * (1.0 / TOTAL_ROWS)
                for v in range(2):
                    rows = pl.ds(v * VIEW, VIEW)
                    out = gpre[d, rows, :] - (
                        total[2 * v:2 * v + 1] + normed[d, rows, :] * total[2 * v + 1:2 * v + 2])
                    scale = gain_ref[:, cols(d)] * inv[1 - g, v, d // RATIO, :, cols(d % RATIO)]
                    grad_out[rows, cols(d)] = (scale * out).astype(BF16)
            if grad:
                values = normed[e]
                pre = gain_ref[:, cols(e)] * values + shift_ref[:, cols(e)]
                vals = jnp.where(pre > 0, vals, 0.0)
                gpre[e] = vals
                stats_put(st, base + e, vals, vals * values)
                stats_send(me, st, ssem, rsem, base + e)
                pl.when(e + 2 < TILES)(lambda: w_copy(e + 2).start())

        def tick(q, carry, g=g, left=left, right=right, grad_step=grad_step, w_copy=w_copy,
                 xh_hbm=xh_hbm):
            p = (1 + g) * PAIRS + q
            lt[...] = left[:, cols(q)].T
            ring.partial(p, lt[...], right)
            ring.send_tick(p)
            each(ring.stage_b)(p)

            @pl.when(q == 0)
            def _():
                if g == 0:
                    lax.fori_loop(1, TILES, out_norm, 0)
                w_copy(0).start()
                w_copy(1).start()
                for copy in normed_copies(xh_hbm, normed_sem):
                    copy.start()

            @pl.when(q == 1)
            def _():
                for copy in normed_copies(xh_hbm, normed_sem):
                    copy.wait()

            def step(e, carry):
                pl.when(e < NORM_LAG)(lambda: grad_step(e, True, False))
                pl.when((e >= NORM_LAG) & (e < TILES))(lambda: grad_step(e, True, True))
                pl.when(e >= TILES)(lambda: grad_step(e, False, True))
                return carry

            @pl.when(q >= 1)
            def _():
                lax.fori_loop((q - 1) * 3 // 2, q * 3 // 2, step, 0)

            if g == 0:
                pl.when(q >= LAG_C)(lambda: each(ring.stage_c)(p - LAG_C))
                pl.when(q >= LAG_D)(lambda: each(store_out)(p - LAG_D))
            else:
                each(ring.stage_c)(p - LAG_C)
                each(store_out)(p - LAG_D)
            return carry

        if g == 1:
            x1_copy.wait()
        lax.fori_loop(0, PAIRS, tick, 0)

    ht[:, view_a] = h_a[...].T
    ht[:, view_b] = h_b[...].T
    per_item = LAST_COLS // TILE

    def rows_of(t):
        return LAST_ROWS if t >= FIRST_LAST else CHUNK

    for t in range(FIRST_LAST, ITEMS + PER * LAG_D):
        if t < ITEMS:
            for m in range(per_item):
                part = dot_nn(ht[...], z[:, cols((t - FIRST_LAST) * per_item + m)])
                for dev in range(8):
                    c, x, y = dev % 2, (dev // 2) % 2, dev // 4
                    a, b = (y, x) if c else (x, y)
                    ring.pa[t % PA_SLOTS, c, a, b, m * PIECE:(m + 1) * PIECE] = part[dev * PIECE:(dev + 1) * PIECE]
            ring.send0(t, LAST_ROWS)
            ring.stage_b(t, LAST_ROWS)
        if t - PER * LAG_C < ITEMS:
            ring.stage_c(t - PER * LAG_C, rows_of(t - PER * LAG_C))
        d = t - PER * LAG_D
        if d < FIRST_LAST:
            store_out(d)
        else:
            total = ring.stage_d(d, LAST_ROWS)
            for m in range(per_item):
                small[pl.ds(0, PIECE), cols((d - FIRST_LAST) * per_item + m)] = total[m * PIECE:(m + 1) * PIECE]
        if t == FIRST_LAST + 4:
            stats_wait(st, ssem, rsem, ST_LOSS)
            loss = jnp.sum(stats_total(st, ST_LOSS), keepdims=True)
            small[pl.ds(PIECE + 4, 4), :] = jnp.broadcast_to(loss, (4, WIDTH))
        if t == FIRST_LAST:
            st[ST_LOSS, 0, pl.ds(0, 1), :] = loss_acc[...]
            stats_send(me, st, ssem, rsem, ST_LOSS)


def finish_kernel(dw3_in, dw2_in, small, dw1, dw2, dw3, gg1, gs1, gg2, gs2, loss, out_sem):
    stores = [(dw3_in, dw3), (dw2_in, dw2), (small.at[pl.ds(0, PIECE)], dw1)]
    for k, ref in enumerate((gs2, gg2, gs1, gg1)):
        stores.append((small.at[pl.ds(PIECE + k, 1), :], ref))
    stores = [pltpu.make_async_copy(src, dst, out_sem.at[k]) for k, (src, dst) in enumerate(stores)]
    for store in stores:
        store.start()
    loss[...] = small[pl.ds(PIECE + 4, 1), pl.ds(0, 1)]
    for store in stores:
        store.wait()


VMEM_SPEC = pl.BlockSpec(memory_space=pltpu.VMEM)
ANY_SPEC = pl.BlockSpec(memory_space=pl.ANY)
SMEM_SPEC = pl.BlockSpec(memory_space=pltpu.SMEM)
DMA = pltpu.SemaphoreType.DMA


def params(collective_id, limit):
    return pltpu.CompilerParams(collective_id=collective_id, has_side_effects=True, vmem_limit_bytes=limit)


def solution(mesh):
    sds = jax.ShapeDtypeStruct
    normed = sds((2, FWD_TILES, VIEW, FWD_TILE), F32)
    act = sds((ROWS, WIDTH), BF16)
    weight = sds((TILE, WIDTH), F32)
    vector = sds((1, WIDTH), F32)
    small = 2 * PIECE - 40
    small_inputs = [pltpu.VMEM((VIEW, FEAT), BF16)] * 2 + [pltpu.VMEM((1, WIDTH), F32)] * 4

    def local_step(h_a, h_b, w_one, w_two, w_three, gain_one, shift_one, gain_two, shift_two, lam_off):
        g1, b1, g2, b2 = (v.reshape(1, WIDTH) for v in (gain_one, shift_one, gain_two, shift_two))
        inv, x1, x2, zh, xh1, xh2, zn = pl.pallas_call(
            forward_kernel,
            out_shape=(sds((3, 2, FWD_TILES, 1, FWD_TILE), F32), act, act, act, normed, normed, normed),
            in_specs=[ANY_SPEC] * 9,
            out_specs=(ANY_SPEC,) * 7,
            scratch_shapes=[
                pltpu.VMEM((ROWS, WIDTH), BF16), pltpu.VMEM((ROWS, WIDTH), BF16), pltpu.VMEM((ROWS, WIDTH), BF16),
                pltpu.VMEM((FEAT, WIDTH), BF16), pltpu.VMEM((2, WIDTH, WIDTH), BF16),
                pltpu.VMEM((2, FWD_TILES, VIEW, FWD_TILE), F32), pltpu.VMEM((6 * FWD_TILES, 8, 2, FWD_TILE), F32),
            ] + small_inputs + [
                pltpu.VMEM((3, 2, FWD_TILES, 1, FWD_TILE), F32), DMA((3, 2)),
                DMA, DMA((2,)), DMA((2, FWD_TILES)), DMA((3, 2, FWD_TILES)), DMA((6 * FWD_TILES,)), DMA((6 * FWD_TILES,)),
                DMA((6,)),
            ],
            compiler_params=params(0, 64_000_000), name="forward",
        )(h_a, h_b, w_one, w_two, w_three, g1, b1, g2, b2)
        dw3, dw2, rest = pl.pallas_call(
            main_kernel,
            out_shape=(pltpu.VMEM((TILE, WIDTH), F32), pltpu.VMEM((TILE, WIDTH), F32), pltpu.VMEM((small, WIDTH), F32)),
            in_specs=[ANY_SPEC] * 15 + [SMEM_SPEC],
            out_specs=(VMEM_SPEC,) * 3,
            scratch_shapes=[
                pltpu.VMEM((ROWS, WIDTH), BF16), pltpu.VMEM((TILES, ROWS, TILE), F32),
                pltpu.VMEM((TILES, ROWS, TILE), F32), pltpu.VMEM((CHUNKS, 2, 2, 2, CHUNK, TILE), BF16),
                pltpu.VMEM((TILE, WIDTH), BF16),
                pltpu.VMEM((ROWS, WIDTH), BF16), pltpu.VMEM((ROWS, WIDTH), BF16), pltpu.VMEM((ROWS, WIDTH), BF16),
                pltpu.VMEM((FEAT, ROWS), BF16), pltpu.VMEM((TILE, ROWS), BF16),
                pltpu.VMEM((2, TILE, WIDTH), BF16),
                pltpu.VMEM((1, TILE), F32), pltpu.VMEM((ST_LOSS + 1, 8, 4, TILE), F32),
            ] + small_inputs + [
                pltpu.VMEM((3, 2, FWD_TILES, 1, FWD_TILE), F32),
                DMA((7,)), DMA((3,)), DMA((2, TILES)), DMA((2,)), DMA((2,)), DMA((ST_LOSS + 1,)), DMA((ST_LOSS + 1,)),
            ] + [DMA((CHUNKS,))] * 6 + RING_SCRATCH,
            compiler_params=params(1, 61_100_000), name="main",
        )(zh, zn, x2, x1, h_a, h_b, w_three, w_two, xh2, xh1, inv, g1, b1, g2, b2, lam_off.reshape(1, 1))
        dw1, dw2, dw3, gg1, gs1, gg2, gs2, loss = pl.pallas_call(
            finish_kernel,
            out_shape=(sds((PIECE, WIDTH), F32), weight, weight, vector, vector, vector, vector, sds((1, 1), F32)),
            in_specs=[VMEM_SPEC] * 3,
            out_specs=(ANY_SPEC,) * 7 + (VMEM_SPEC,),
            scratch_shapes=[DMA((7,))],
            compiler_params=pltpu.CompilerParams(vmem_limit_bytes=16_000_000), name="finish",
        )(dw3, dw2, rest)
        return (loss.reshape(()), dw1, dw2, dw3, gg1.reshape(WIDTH), gs1.reshape(WIDTH),
                gg2.reshape(WIDTH), gs2.reshape(WIDTH))

    row_spec = P("data", None)
    whole_mat = P(None, None)
    whole_vec = P(None)
    return jax.shard_map(
        local_step, mesh=mesh,
        in_specs=(row_spec, row_spec, whole_mat, whole_mat, whole_mat,
                  whole_vec, whole_vec, whole_vec, whole_vec, P()),
        out_specs=(P(), row_spec, row_spec, row_spec, whole_vec, whole_vec, whole_vec, whole_vec),
        check_vma=False)
```
